16 devices in a mesh: etp: 4 (over z, y), ep: 4 (over x, core).
Axes of the slice: x: 2, y: 2, z: 2, core: 2. Of those that a mesh axis runs over, the one named last changes fastest.
Arguments:
- hidden: bfloat16 [32768, 768], P(('ep', 'etp'))
- w_router: float32 [768, 8], replicated
- expert_ids: int32 [32768, 2], P(('ep', 'etp'))
- d_out: bfloat16 [32768, 768], P(('ep', 'etp'))
- w_gate: bfloat16 [8, 768, 4096], P('ep', None, 'etp')
- w_up: bfloat16 [8, 768, 4096], P('ep', None, 'etp')
- w_down: bfloat16 [8, 4096, 768], P('ep', 'etp')
Outputs:
- output 1: bfloat16 [32768, 768], P(('ep', 'etp'))
- output 2: bfloat16 [32768, 768], P(('ep', 'etp'))
- output 3: float32 [768, 8], replicated
- output 4: float32 [], replicated
- output 5: float32 [8, 768, 4096], P('ep', None, 'etp')
- output 6: float32 [8, 768, 4096], P('ep', None, 'etp')
- output 7: float32 [8, 4096, 768], P('ep', 'etp')
All inputs are finite; a program needn't handle non-finite values.
Results may differ from the reference program's by a relative error of at most 0.0089382.
Values are sent between devices in bfloat16 or wider.
A program may use at most 1 GiB of HBM per device.

```python
import jax
import jax.numpy as jnp
from jax import lax

EXPERTS = 8
D_MODEL = 768
D_FF = 4096
TOKENS = 32768
N_DEVICES = 16

CAPACITY = (5 * TOKENS + 2 * EXPERTS - 1) // (2 * EXPERTS)
BLOCK_TOKENS = TOKENS // N_DEVICES


def draw_choices(draw_key):
    quarter = BLOCK_TOKENS // (2 * EXPERTS)
    perm_key, block_key = jax.random.split(draw_key)
    expert_order = jax.random.permutation(perm_key, EXPERTS)
    hot_shift = jnp.zeros((EXPERTS,), jnp.int32).at[:4].set(jnp.array([2, 2, -2, -2], jnp.int32) * quarter)

    def one_block(one_key):
        k_noise, k_rows, k_flip = jax.random.split(one_key, 3)
        count_noise = jax.random.randint(k_noise, (EXPERTS,), 0, quarter + 1)
        count_noise = count_noise.at[0].set(quarter).at[1].set(0)
        count_perm = 4 * quarter + count_noise - jnp.roll(count_noise, -1) + hot_shift
        counts = jnp.zeros((EXPERTS,), jnp.int32).at[expert_order].set(count_perm)
        ends = jnp.cumsum(counts)
        id_seq = jnp.sum(jnp.arange(2 * BLOCK_TOKENS)[:, None] >= ends[None, :], axis=1).astype(jnp.int32)
        id_pairs = jnp.stack([id_seq[:BLOCK_TOKENS], id_seq[BLOCK_TOKENS:]], axis=1)
        id_pairs = id_pairs[jax.random.permutation(k_rows, BLOCK_TOKENS)]
        flip_mask = jax.random.randint(k_flip, (BLOCK_TOKENS, 1), 0, 2) == 1
        return jnp.where(flip_mask, id_pairs[:, ::-1], id_pairs)

    blocks = jax.vmap(one_block)(jax.random.split(block_key, N_DEVICES))
    return blocks.reshape(TOKENS, 2)


def setup_inputs(seed: int = 0) -> dict:
    root_key = jax.random.key(seed)
    k_hid, k_route, k_ids, k_dout, k_gate, k_up, k_down = jax.random.split(root_key, 7)
    hidden = jax.random.normal(k_hid, (TOKENS, D_MODEL), jnp.float32).astype(jnp.bfloat16)
    w_router = jax.random.normal(k_route, (D_MODEL, EXPERTS), jnp.float32) * (0.5 * D_MODEL ** -0.5)
    expert_ids = draw_choices(k_ids)
    d_out = jax.random.normal(k_dout, (TOKENS, D_MODEL), jnp.float32).astype(jnp.bfloat16)
    w_gate = (jax.random.normal(k_gate, (EXPERTS, D_MODEL, D_FF), jnp.float32) * D_MODEL ** -0.5).astype(jnp.bfloat16)
    w_up = (jax.random.normal(k_up, (EXPERTS, D_MODEL, D_FF), jnp.float32) * D_MODEL ** -0.5).astype(jnp.bfloat16)
    w_down = (jax.random.normal(k_down, (EXPERTS, D_FF, D_MODEL), jnp.float32) * D_FF ** -0.5).astype(jnp.bfloat16)
    return {"hidden": hidden, "w_router": w_router, "expert_ids": expert_ids, "d_out": d_out, "w_gate": w_gate, "w_up": w_up, "w_down": w_down}


def route_terms(logits, expert_ids):
    prob_vals = jax.nn.softmax(logits, axis=-1)
    picked = jnp.take_along_axis(prob_vals, expert_ids, axis=1)
    return picked / jnp.sum(picked, axis=1, keepdims=True), jnp.sum(prob_vals, axis=0)


def expert_pass(operands):
    x_buf, dy_buf, gate_w, up_w, down_w = operands
    act_a = jnp.dot(x_buf, gate_w, preferred_element_type=jnp.float32)
    act_b = jnp.dot(x_buf, up_w, preferred_element_type=jnp.float32)
    sig_a = jax.nn.sigmoid(act_a)
    silu_a = act_a * sig_a
    inner_act = (silu_a * act_b).astype(jnp.bfloat16)
    y_buf = jnp.dot(inner_act, down_w, preferred_element_type=jnp.float32).astype(jnp.bfloat16)
    d_inner = jnp.dot(dy_buf, down_w.T, preferred_element_type=jnp.float32)
    d_act_a = (d_inner * act_b * sig_a * (1.0 + act_a * (1.0 - sig_a))).astype(jnp.bfloat16)
    d_act_b = (d_inner * silu_a).astype(jnp.bfloat16)
    dx_buf = (jnp.dot(d_act_a, gate_w.T, preferred_element_type=jnp.float32) + jnp.dot(d_act_b, up_w.T, preferred_element_type=jnp.float32)).astype(jnp.bfloat16)
    g_gate = jnp.dot(x_buf.T, d_act_a, preferred_element_type=jnp.float32)
    g_up = jnp.dot(x_buf.T, d_act_b, preferred_element_type=jnp.float32)
    g_down = jnp.dot(inner_act.T, dy_buf, preferred_element_type=jnp.float32)
    return y_buf, dx_buf, g_gate, g_up, g_down


def reference(hidden, w_router, expert_ids, d_out, w_gate, w_up, w_down):
    hidden_f = hidden.astype(jnp.float32)
    logits = jnp.dot(hidden_f, w_router, preferred_element_type=jnp.float32)
    (gate_vals, prob_sum), route_vjp = jax.vjp(lambda logit_in: route_terms(logit_in, expert_ids), logits)
    n_assign = 2 * TOKENS
    flat_ids = expert_ids.reshape(-1)
    assign = jnp.arange(n_assign, dtype=jnp.int32)
    counts = jnp.bincount(flat_ids, length=EXPERTS)
    sort_order = jnp.argsort(flat_ids * n_assign + assign)
    sort_rank = jnp.zeros((n_assign,), jnp.int32).at[sort_order].set(assign)
    starts = jnp.cumsum(counts) - counts
    slot_pos = sort_rank - starts[flat_ids]
    dest_rows = jnp.where(slot_pos < CAPACITY, flat_ids * CAPACITY + slot_pos, EXPERTS * CAPACITY)
    source = jnp.full((EXPERTS * CAPACITY,), n_assign, jnp.int32).at[dest_rows].set(assign, mode="drop")
    x_buf = jnp.take(hidden, source // 2, axis=0, mode="fill", fill_value=0).reshape(EXPERTS, CAPACITY, D_MODEL)
    d_mix = 2.0 * d_out.astype(jnp.float32)
    dy_assign = (gate_vals[:, :, None] * d_mix[:, None, :]).astype(jnp.bfloat16).reshape(n_assign, D_MODEL)
    dy_buf = jnp.take(dy_assign, source, axis=0, mode="fill", fill_value=0).reshape(EXPERTS, CAPACITY, D_MODEL)
    y_buf, dx_buf, g_gate, g_up, g_down = lax.map(expert_pass, (x_buf, dy_buf, w_gate, w_up, w_down))
    y_pair = jnp.take(y_buf.reshape(EXPERTS * CAPACITY, D_MODEL), dest_rows, axis=0, mode="fill", fill_value=0).reshape(TOKENS, 2, D_MODEL).astype(jnp.float32)
    dx_pair = jnp.take(dx_buf.reshape(EXPERTS * CAPACITY, D_MODEL), dest_rows, axis=0, mode="fill", fill_value=0).reshape(TOKENS, 2, D_MODEL).astype(jnp.float32)
    output = (hidden_f + 2.0 * jnp.sum(gate_vals[:, :, None] * y_pair, axis=1)).astype(jnp.bfloat16)
    d_gates = jnp.sum(d_mix[:, None, :] * y_pair, axis=2)
    route_frac = counts.astype(jnp.float32) / n_assign
    aux_loss = 0.01 * EXPERTS * jnp.sum(route_frac * prob_sum) / TOKENS
    (d_logits,) = route_vjp((d_gates, (0.01 * EXPERTS / TOKENS) * route_frac))
    d_router = jnp.dot(hidden_f.T, d_logits, preferred_element_type=jnp.float32)
    d_hidden = (d_out.astype(jnp.float32) + jnp.sum(dx_pair, axis=1) + jnp.dot(d_logits, w_router.T, preferred_element_type=jnp.float32)).astype(jnp.bfloat16)
    return output, d_hidden, d_router, aux_loss, g_gate, g_up, g_down
```

```python
import functools
import jax
import jax.numpy as jnp
import numpy as np
from jax import lax
from jax.experimental import pallas as pl
from jax.experimental.pallas import tpu as pltpu
from jax.sharding import PartitionSpec as P

AUX_COEF = 0.01
OUT_SCALE = 2.0
BF16 = jnp.bfloat16
F32 = jnp.float32
I32 = jnp.int32
VMEM_LIMIT = 62 * 1024 * 1024


N_SHIFT = 8
TOK_TILE = 256
ROW_TILE = 512
ALIGN = 16
WIN = TOK_TILE + ALIGN


def coords(i):
    return (i >> 3) & 1, (i >> 2) & 1, (i >> 1) & 1, i & 1


def index_of(z, y, x, c):
    return (z << 3) | (y << 2) | (x << 1) | c


def shift_dest(i, s):
    z, y, x, c = coords(i)
    x, c, d = x ^ ((s >> 2) & 1), c ^ ((s >> 1) & 1), s & 1
    return index_of(z, y ^ d, x, c) if c == 0 else index_of(z ^ d, y, x, c)


def split_partner(i):
    z, y, x, c = coords(i)
    return index_of(z, y ^ 1, x, c) if c == 0 else index_of(z ^ 1, y, x, c)


def twin_partner(i):
    z, y, x, c = coords(i)
    return index_of(z ^ 1, y, x, c) if c == 0 else index_of(z, y ^ 1, x, c)


def dot_nn(a, b):
    return lax.dot_general(a, b, (((1,), (0,)), ((), ())), preferred_element_type=F32)


def dot_nt(a, b):
    return lax.dot_general(a, b, (((1,), (1,)), ((), ())), preferred_element_type=F32)


def dot_tn(a, b):
    return lax.dot_general(a, b, (((0,), (0,)), ((), ())), preferred_element_type=F32)


def iota(shape, dim):
    return lax.broadcasted_iota(I32, shape, dim)


def tile_columns(ids_t, starts, limits, n_experts, upper):
    tokens = ids_t.shape[1]
    e_iota = iota((n_experts, tokens), 0)
    hot0 = ids_t[0:1, :] == e_iota
    hot1 = ids_t[1:2, :] == e_iota
    either = jnp.where(hot0 | hot1, 1.0, 0.0).astype(BF16)
    before = dot_nn(either, upper).astype(I32)
    offset = jnp.zeros((n_experts, tokens), I32)
    bound = jnp.zeros((n_experts, tokens), I32)
    for e in range(n_experts):
        offset = jnp.where(e_iota == e, e * WIN + (starts[e] & (ALIGN - 1)), offset)
        if limits is not None:
            bound = jnp.where(e_iota == e, limits[e] - starts[e], bound)
    column = before + offset
    if limits is not None:
        column = jnp.where(before < bound, column, -1)
    return [jnp.sum(jnp.where(hot, column, 0), axis=0, keepdims=True) for hot in (hot0, hot1)]


def strict_upper(n):
    return jnp.where(iota((n, n), 0) < iota((n, n), 1), 1.0, 0.0).astype(BF16)


def add_windows(buf, value, starts, n_experts):
    for e in range(n_experts):
        rows = pl.ds(pl.multiple_of(starts[e] - (starts[e] & (ALIGN - 1)), ALIGN), WIN)
        buf[e, rows, :] = buf[e, rows, :] + value[e * WIN:(e + 1) * WIN, :]


def slots_out(buf, order_ref, outs, sem):
    slots = outs[0].shape[0]
    copies = [pltpu.make_async_copy(buf.at[order_ref[s], pl.ds(0, slots), :], outs[s], sem.at[s]) for s in range(N_SHIFT)]
    for copy in copies:
        copy.start()
    for copy in copies:
        copy.wait()


def x_slots_kernel(order_ref, ids_ref, h_ref, base_ref, *rest):
    outs, (buf, base_s, sem, base_sem) = rest[:N_SHIFT], rest[N_SHIFT:]
    n_experts, tokens = base_ref.shape[0], ids_ref.shape[1]
    e_iota = iota((n_experts, tokens), 0)
    hot = (ids_ref[0:1, :] == e_iota) | (ids_ref[1:2, :] == e_iota)
    earlier = jnp.where(iota((tokens, 128), 0) < TOK_TILE * iota((tokens, 128), 1), 1.0, 0.0).astype(BF16)
    base_ref[...] = dot_nn(jnp.where(hot, 1.0, 0.0).astype(BF16), earlier).astype(I32)
    copy = pltpu.make_async_copy(base_ref, base_s, base_sem)
    copy.start()
    buf[...] = jnp.zeros_like(buf)
    copy.wait()
    upper = strict_upper(TOK_TILE)

    @pl.loop(0, tokens // TOK_TILE)
    def _(t):
        here = pl.ds(pl.multiple_of(t * TOK_TILE, TOK_TILE), TOK_TILE)
        starts = [base_s[e, t] for e in range(n_experts)]
        col0, col1 = tile_columns(ids_ref[:, here], starts, None, n_experts, upper)
        row = iota((n_experts * WIN, TOK_TILE), 0)
        pick = jnp.where((row == col0) | (row == col1), 1.0, 0.0).astype(BF16)
        add_windows(buf, dot_nn(pick, h_ref[here, :]).astype(BF16), starts, n_experts)

    slots_out(buf, order_ref, outs, sem)


def c_slots_kernel(order_ref, base_s, limit_s, ids_ref, h_ref, dy_ref, wr3_ref, info_ref, psum_ref, *rest):
    outs, (buf, prob_buf, sem) = rest[:N_SHIFT], rest[N_SHIFT:]
    n_experts, tokens = psum_ref.shape[0], ids_ref.shape[1]
    parts = dot_nt(wr3_ref[...], h_ref[...])
    logits = parts[2 * n_experts:3 * n_experts] + parts[n_experts:2 * n_experts] + parts[0:n_experts]
    top = jnp.max(logits, axis=0, keepdims=True)
    expo = jnp.exp(logits - top)
    prob = expo / jnp.sum(expo, axis=0, keepdims=True)
    prob_buf[...] = prob
    psum_ref[...] = jnp.broadcast_to(jnp.sum(prob, axis=1, keepdims=True), psum_ref.shape)
    buf[...] = jnp.zeros_like(buf)
    upper = strict_upper(TOK_TILE)
    limits = [limit_s[e] for e in range(n_experts)]

    @pl.loop(0, tokens // TOK_TILE)
    def _(t):
        here = pl.ds(pl.multiple_of(t * TOK_TILE, TOK_TILE), TOK_TILE)
        starts = [base_s[e, t] for e in range(n_experts)]
        ids_t = ids_ref[:, here]
        p_t = prob_buf[:, here]
        e_iota = iota((n_experts, TOK_TILE), 0)
        p0 = jnp.sum(jnp.where(ids_t[0:1, :] == e_iota, p_t, 0.0), axis=0, keepdims=True)
        p1 = jnp.sum(jnp.where(ids_t[1:2, :] == e_iota, p_t, 0.0), axis=0, keepdims=True)
        total = p0 + p1
        g0, g1 = p0 / total, p1 / total
        col0, col1 = tile_columns(ids_t, starts, limits, n_experts, upper)
        row = iota((n_experts * WIN, TOK_TILE), 0)
        is0, is1 = row == col0, row == col1
        pick = jnp.where(is0 | is1, 1.0, 0.0).astype(BF16)
        gate = jnp.sum(jnp.where(is0, g0, jnp.where(is1, g1, 0.0)), axis=1, keepdims=True)
        mixed = OUT_SCALE * dot_nn(pick, dy_ref[here, :])
        add_windows(buf, (gate * mixed).astype(BF16), starts, n_experts)
        group = iota((8, TOK_TILE), 0)
        extra = jnp.zeros((8, TOK_TILE), F32)
        for k, v in enumerate((g0, g1, col0.astype(F32), col1.astype(F32), ids_t[0:1, :].astype(F32), ids_t[1:2, :].astype(F32))):
            extra = jnp.where(group == k, v, extra)
        table = jnp.concatenate([p_t] * 6 + [extra, jnp.zeros((128 - 6 * n_experts - 8, TOK_TILE), F32)], axis=0)
        info_ref[here, :] = table.T

    slots_out(buf, order_ref, outs, sem)


def pack_kernel(count_s, offset_s, *refs):
    ins, out_ref, (buf, sem, out_sem) = refs[:N_SHIFT], refs[N_SHIFT], refs[N_SHIFT + 1:]
    sizes = [512, 256, 128, 64, 32, 16]

    def for_parts(act):
        for s in range(N_SHIFT):
            count, offset = count_s[s], offset_s[s]
            done = jnp.int32(0)
            for j, size in enumerate(sizes):
                has = (count & size) != 0
                start = pl.multiple_of(done, ALIGN)
                dest = pl.multiple_of(offset + done, ALIGN)

                @pl.when(has)
                def _(s=s, j=j, size=size, start=start, dest=dest):
                    act(pltpu.make_async_copy(ins[s].at[pl.ds(start, size), :], buf.at[pl.ds(dest, size), :], sem.at[s, j]))

                done = done + jnp.where(has, size, 0)

    for_parts(lambda copy: copy.start())
    total = pl.multiple_of(offset_s[N_SHIFT], ALIGN)
    buf[pl.ds(total, ROW_TILE), :] = jnp.zeros((ROW_TILE, buf.shape[1]), buf.dtype)
    for_parts(lambda copy: copy.wait())
    copy = pltpu.make_async_copy(buf.at[pl.ds(0, out_ref.shape[0]), :], out_ref, out_sem)
    copy.start()
    copy.wait()


def rows_out(buf, offset_s, outs, sem):
    slots = outs[0].shape[0]
    copies = [pltpu.make_async_copy(buf.at[pl.ds(pl.multiple_of(offset_s[s], ALIGN), slots), :], outs[s], sem.at[s]) for s in range(N_SHIFT)]
    for copy in copies:
        copy.start()
    for copy in copies:
        copy.wait()


def forward_kernel(n_ref, offset_s, x_ref, w1_ref, w3_ref, w2_ref, *rest, first, last):
    rest = list(rest)
    y_in = None if first else rest.pop(0)
    a_ref, b_ref = rest.pop(0), rest.pop(0)
    if last:
        outs, (buf, sem) = rest[:N_SHIFT], rest[N_SHIFT:]
    else:
        (y_out,) = rest
    i = pl.program_id(0)

    @pl.when(i < n_ref[0])
    def _():
        a = dot_nn(x_ref[...], w1_ref[...])
        b = dot_nn(x_ref[...], w3_ref[...])
        a_ref[...] = a
        b_ref[...] = b
        y = dot_nn((a * jax.nn.sigmoid(a) * b).astype(BF16), w2_ref[...])
        if not first:
            y = y_in[...] + y
        if last:
            buf[pl.ds(pl.multiple_of(i * ROW_TILE, ROW_TILE), ROW_TILE), :] = y.astype(BF16)
        else:
            y_out[...] = y

    if last:
        @pl.when(i == pl.num_programs(0) - 1)
        def _():
            rows_out(buf, offset_s, outs, sem)


def backward_kernel(n_ref, offset_s, x_ref, c_ref, a_ref, b_ref, w1_ref, w3_ref, w2_ref, *rest, first, last):
    rest = list(rest)
    dx_in = None if first else rest.pop(0)
    g1_ref, g3_ref, g2_ref = rest.pop(0), rest.pop(0), rest.pop(0)
    if last:
        outs, (buf, sem) = rest[:N_SHIFT], rest[N_SHIFT:]
    else:
        (dx_out,) = rest
    i = pl.program_id(0)

    @pl.when(i == 0)
    def _():
        g1_ref[...] = jnp.zeros_like(g1_ref)
        g3_ref[...] = jnp.zeros_like(g3_ref)
        g2_ref[...] = jnp.zeros_like(g2_ref)

    @pl.when(i < n_ref[0])
    def _():
        du = dot_nt(c_ref[...], w2_ref[...])
        a, b = a_ref[...], b_ref[...]
        sig = jax.nn.sigmoid(a)
        silu = a * sig
        da = (du * b * sig * (1.0 + a * (1.0 - sig))).astype(BF16)
        db = (du * silu).astype(BF16)
        u = (silu * b).astype(BF16)
        dx = dot_nt(da, w1_ref[...]) + dot_nt(db, w3_ref[...])
        if not first:
            dx = dx_in[...] + dx
        if last:
            buf[pl.ds(pl.multiple_of(i * ROW_TILE, ROW_TILE), ROW_TILE), :] = dx.astype(BF16)
        else:
            dx_out[...] = dx
        g1_ref[...] += dot_tn(x_ref[...], da)
        g3_ref[...] += dot_tn(x_ref[...], db)
        g2_ref[...] += dot_tn(u, c_ref[...])

    if last:
        @pl.when(i == pl.num_programs(0) - 1)
        def _():
            rows_out(buf, offset_s, outs, sem)


def load_slots(order_ref, ins, buf, sem):
    slots = ins[0].shape[0]
    copies = [pltpu.make_async_copy(ins[s], buf.at[order_ref[s], pl.ds(0, slots), :], sem.at[s]) for s in range(N_SHIFT)]
    for copy in copies:
        copy.start()
    for copy in copies:
        copy.wait()


def gather_windows(buf, window, base_s, kept_s, t, n_experts):
    for e in range(n_experts):
        start = base_s[e, t] - (base_s[e, t] & (ALIGN - 1))
        rows = buf[e, pl.ds(pl.multiple_of(start, ALIGN), WIN), :]
        valid = iota(rows.shape, 0) < kept_s[e] - start
        window[e * WIN:(e + 1) * WIN, :] = jnp.where(valid, rows, jnp.zeros_like(rows))


def y_combine_kernel(order_ref, base_s, kept_s, *refs):
    ins, refs = refs[:N_SHIFT], refs[N_SHIFT:]
    info_ref, h_ref, dy_ref, w_ref, out_ref, dz_ref, dwr_ref, buf, window, sem = refs
    n_experts = buf.shape[0]
    t = pl.program_id(0)

    @pl.when(t == 0)
    def _():
        load_slots(order_ref, ins, buf, sem)
        dwr_ref[...] = jnp.zeros_like(dwr_ref)

    gather_windows(buf, window, base_s, kept_s, t, n_experts)
    info = info_ref[...]
    k0 = 6 * n_experts
    g0, g1, col0, col1, e0, e1 = [info[:, k0 + k:k0 + k + 1] for k in range(6)]
    col = iota((TOK_TILE, n_experts * WIN), 1)
    pick0 = jnp.where(col == col0.astype(I32), 1.0, 0.0).astype(BF16)
    pick1 = jnp.where(col == col1.astype(I32), 1.0, 0.0).astype(BF16)
    y0 = dot_nn(pick0, window[...])
    y1 = dot_nn(pick1, window[...])
    h = h_ref[...]
    mix = OUT_SCALE * dy_ref[...].astype(F32)
    out_ref[...] = (h.astype(F32) + OUT_SCALE * (g0 * y0 + g1 * y1)).astype(BF16)
    dg0 = jnp.sum(mix * y0, axis=1, keepdims=True)
    dg1 = jnp.sum(mix * y1, axis=1, keepdims=True)
    lane = iota(info.shape, 1)
    prob = jnp.where(lane < k0, info, 0.0)
    weight = w_ref[...]
    mean_w = jnp.sum(jnp.where(lane < n_experts, prob * weight, 0.0), axis=1, keepdims=True)
    expert = (lane & (n_experts - 1)).astype(F32)
    sign = jnp.where(expert == e0, 1.0, 0.0) - jnp.where(expert == e1, 1.0, 0.0)
    dz = prob * (weight - mean_w) + g0 * g1 * (dg0 - dg1) * jnp.where(lane < k0, sign, 0.0)
    d1 = dz.astype(BF16)
    rem1 = dz - d1.astype(F32)
    d2 = rem1.astype(BF16)
    d3 = (rem1 - d2.astype(F32)).astype(BF16)
    group = lane // n_experts
    first = (group == 0) | (group == 1) | (group == 3)
    second = (group == 2) | (group == 4)
    dzp = jnp.where(first, d1.astype(F32), jnp.where(second, d2.astype(F32), d3.astype(F32))).astype(BF16)
    dz_ref[...] = dzp
    dwr_ref[...] += dot_tn(dzp, h)


def dx_combine_kernel(order_ref, base_s, kept_s, *refs):
    ins, refs = refs[:N_SHIFT], refs[N_SHIFT:]
    info_ref, dz_ref, dy_ref, wr_ref, out_ref, buf, window, sem = refs
    n_experts = buf.shape[0]
    t = pl.program_id(0)

    @pl.when(t == 0)
    def _():
        load_slots(order_ref, ins, buf, sem)

    gather_windows(buf, window, base_s, kept_s, t, n_experts)
    info = info_ref[...]
    k0 = 6 * n_experts
    col0, col1 = info[:, k0 + 2:k0 + 3].astype(I32), info[:, k0 + 3:k0 + 4].astype(I32)
    col = iota((TOK_TILE, n_experts * WIN), 1)
    pick = jnp.where((col == col0) | (col == col1), 1.0, 0.0).astype(BF16)
    total = dy_ref[...].astype(F32) + dot_nn(pick, window[...]) + dot_nn(dz_ref[...], wr_ref[...])
    out_ref[...] = total.astype(BF16)


def finish_kernel(j_ref, own_ref, part_ref, other_ref, out_ref):
    own = pl.program_id(0) == j_ref[0]

    @pl.when(own)
    def _():
        out_ref[0] = own_ref[...] + part_ref[...]

    @pl.when(jnp.logical_not(own))
    def _():
        out_ref[0] = other_ref[...]


def params(*semantics):
    return pltpu.CompilerParams(dimension_semantics=semantics or None, vmem_limit_bytes=VMEM_LIMIT)


def hbm():
    return pl.BlockSpec(memory_space=pl.ANY)


def smem():
    return pl.BlockSpec(memory_space=pltpu.SMEM)


def vmem():
    return pl.BlockSpec(memory_space=pltpu.VMEM)


def cost(flops, nbytes):
    return pl.CostEstimate(flops=int(flops), bytes_accessed=int(nbytes), transcendentals=0)


def split3(v):
    p1 = v.astype(BF16)
    r1 = v - p1.astype(F32)
    p2 = r1.astype(BF16)
    return p1, p2, (r1 - p2.astype(F32)).astype(BF16)


def solution(mesh):
    ep_size = mesh.shape["ep"]
    etp_size = mesh.shape["etp"]
    n_dev = ep_size * etp_size
    all_axes = ("ep", "etp")
    dev_axes = ("etp", "ep")
    tok_spec = P(all_axes, None)
    gate_spec = P("ep", None, "etp")
    down_spec = P("ep", "etp", None)

    def layer(hidden, w_router, expert_ids, d_out, w_gate, w_up, w_down):
        tok_rows, d_model = hidden.shape
        n_experts = w_router.shape[1]
        n_tokens = tok_rows * n_dev
        capacity = (5 * n_tokens + 2 * n_experts - 1) // (2 * n_experts)
        slots = 7 * tok_rows // (2 * n_experts)
        width = w_gate.shape[2]
        rows = N_SHIFT * slots
        buf_rows = slots + WIN + ALIGN
        etp, ep = lax.axis_index("etp"), lax.axis_index("ep")
        z, y, x, c = etp >> 1, etp & 1, ep >> 1, ep & 1
        mine = jnp.where(c == 0, y, z)

        def permute(values, pairs):
            return [lax.ppermute(v, dev_axes, pairs) for v in values]

        forth = [[(i, shift_dest(i, s)) for i in range(n_dev)] for s in range(N_SHIFT)]
        back = [[(b, a) for a, b in pairs] for pairs in forth]
        split_pairs = [(i, split_partner(i)) for i in range(n_dev)]
        twin_pairs = [(i, twin_partner(i)) for i in range(n_dev)]

        order = []
        source = []
        for s in range(N_SHIFT):
            dx, dc, d = (s >> 2) & 1, (s >> 1) & 1, s & 1
            order.append(4 * (x ^ dx) + 2 * (c ^ dc) + (jnp.where((c ^ dc) == 0, y, z) ^ d))
            sx, sc = x ^ dx, c ^ dc
            sz = jnp.where(c == 0, z, z ^ d)
            sy = jnp.where(c == 0, y ^ d, y)
            source.append((sx * 2 + sc) * etp_size + sz * 2 + sy)
        order = jnp.stack(order).astype(I32)
        source = jnp.stack(source).astype(I32)

        ids_t = expert_ids.T
        slot_shape = jax.ShapeDtypeStruct((slots, d_model), BF16)
        slot_buf = pltpu.VMEM((n_experts, buf_rows, d_model), BF16)
        dma8 = pltpu.SemaphoreType.DMA((N_SHIFT,))
        spread_flops = 2 * tok_rows * n_experts * WIN * d_model

        base, *x_send = pl.pallas_call(
            x_slots_kernel,
            in_specs=[smem(), vmem(), vmem()],
            out_specs=[vmem()] + [hbm()] * N_SHIFT,
            out_shape=[jax.ShapeDtypeStruct((n_experts, 128), I32)] + [slot_shape] * N_SHIFT,
            scratch_shapes=[slot_buf, pltpu.SMEM((n_experts, 128), I32), dma8, pltpu.SemaphoreType.DMA],
            compiler_params=params(), cost_estimate=cost(spread_flops, 2 * rows * d_model), name="x_slots",
        )(order, ids_t, hidden)
        x_recv = [x_send[0]] + [lax.ppermute(x_send[s], dev_axes, forth[s]) for s in range(1, N_SHIFT)]

        counts = base[:, tok_rows // TOK_TILE]
        count_table = lax.all_gather(counts, all_axes)
        running = jnp.cumsum(count_table, axis=0) - count_table
        total_count = jnp.sum(count_table, axis=0)
        block_idx = ep * etp_size + etp
        limit = jnp.clip(capacity - running, 0, None)
        kept_table = jnp.minimum(count_table, limit)
        my_limit, my_kept = limit[block_idx], kept_table[block_idx]
        my_expert = order[0]
        part = (kept_table[source, my_expert] + ALIGN - 1) // ALIGN * ALIGN
        offset = jnp.concatenate([jnp.zeros((1,), I32), jnp.cumsum(part)]).astype(I32)
        n_tiles = (offset[N_SHIFT:] + ROW_TILE - 1) // ROW_TILE

        wr_t = split3(w_router.T)
        wr3 = jnp.concatenate(wr_t + (jnp.zeros_like(wr_t[0]),), axis=0)
        wr6 = jnp.concatenate([wr_t[0], wr_t[1], wr_t[0], wr_t[2], wr_t[1], wr_t[0], jnp.zeros((128 - 6 * n_experts, d_model), BF16)], axis=0)
        info, prob_sum, *c_send = pl.pallas_call(
            c_slots_kernel,
            in_specs=[smem()] * 3 + [vmem()] * 4,
            out_specs=[vmem()] * 2 + [hbm()] * N_SHIFT,
            out_shape=[jax.ShapeDtypeStruct((tok_rows, 128), F32), jax.ShapeDtypeStruct((n_experts, 128), F32)] + [slot_shape] * N_SHIFT,
            scratch_shapes=[slot_buf, pltpu.VMEM((n_experts, tok_rows), F32), dma8],
            compiler_params=params(), cost_estimate=cost(spread_flops, 2 * rows * d_model), name="c_slots",
        )(order, base, my_limit, ids_t, hidden, d_out, wr3)

        def take(w, j):
            return lax.dynamic_index_in_dim(w, j, 0, keepdims=False)

        weights = (w_gate, w_up, w_down)
        q_own = [take(w, mine) for w in weights]
        q_split = permute([take(w, 1 - mine) for w in weights], split_pairs)
        q_twin = permute(q_own, twin_pairs)
        q_far = permute(q_split, twin_pairs)

        c_recv = [c_send[0]] + [lax.ppermute(c_send[s], dev_axes, forth[s]) for s in range(1, N_SHIFT)]

        def pack(parts, name):
            return pl.pallas_call(
                pack_kernel,
                in_specs=[smem()] * 2 + [hbm()] * N_SHIFT,
                out_specs=hbm(),
                out_shape=jax.ShapeDtypeStruct((rows, d_model), BF16),
                scratch_shapes=[pltpu.VMEM((rows + ROW_TILE, d_model), BF16), pltpu.SemaphoreType.DMA((N_SHIFT, 6)), pltpu.SemaphoreType.DMA],
                compiler_params=params(), cost_estimate=cost(10**9, 4 * rows * d_model), name=name,
            )(part, offset, *parts)

        def row_spec(w):
            return pl.BlockSpec((ROW_TILE, w), lambda i, n, o: (jnp.clip(n[0] - 1, 0, i), 0))

        def full_spec(shape):
            return pl.BlockSpec(shape, lambda i, n, o: (0, 0), pipeline_mode=pl.Buffered(1))

        grid = (rows // ROW_TILE,)
        up_shape, down_shape = (d_model, width), (width, d_model)
        row_f32 = jax.ShapeDtypeStruct((rows, d_model), F32)
        act_shape = jax.ShapeDtypeStruct((rows, width), F32)
        row_buf = pltpu.VMEM((rows + slots, d_model), BF16)
        mm = 2 * rows * d_model * width

        def forward(quarter, y_acc, first, last):
            n_in = 4 + (not first)
            out = pl.pallas_call(
                functools.partial(forward_kernel, first=first, last=last),
                grid_spec=pltpu.PrefetchScalarGridSpec(
                    num_scalar_prefetch=2, grid=grid,
                    in_specs=[row_spec(d_model), full_spec(up_shape), full_spec(up_shape), full_spec(down_shape)] + [row_spec(d_model)] * (not first),
                    out_specs=[row_spec(width)] * 2 + ([hbm()] * N_SHIFT if last else [row_spec(d_model)]),
                    scratch_shapes=[row_buf, dma8] if last else []),
                out_shape=[act_shape] * 2 + ([slot_shape] * N_SHIFT if last else [row_f32]),
                input_output_aliases={} if first or last else {2 + n_in - 1: 2},
                compiler_params=params("arbitrary"), cost_estimate=cost(3 * mm, 20 * rows * d_model), name="forward",
            )(n_tiles, offset, x_rows, *quarter, *([] if first else [y_acc]))
            return out[0], out[1], (out[2:] if last else out[2])

        def backward(quarter, acts, dx_acc, first, last):
            n_in = 7 + (not first)
            out = pl.pallas_call(
                functools.partial(backward_kernel, first=first, last=last),
                grid_spec=pltpu.PrefetchScalarGridSpec(
                    num_scalar_prefetch=2, grid=grid,
                    in_specs=[row_spec(d_model)] * 2 + [row_spec(width)] * 2 + [full_spec(up_shape), full_spec(up_shape), full_spec(down_shape)] + [row_spec(d_model)] * (not first),
                    out_specs=[full_spec(up_shape), full_spec(up_shape), full_spec(down_shape)] + ([hbm()] * N_SHIFT if last else [row_spec(d_model)]),
                    scratch_shapes=[row_buf, dma8] if last else []),
                out_shape=[jax.ShapeDtypeStruct(up_shape, F32)] * 2 + [jax.ShapeDtypeStruct(down_shape, F32)] + ([slot_shape] * N_SHIFT if last else [row_f32]),
                input_output_aliases={} if first or last else {2 + n_in - 1: 3},
                compiler_params=params("arbitrary"), cost_estimate=cost(6 * mm, 20 * rows * d_model), name="backward",
            )(n_tiles, offset, x_rows, c_rows, *acts, *quarter, *([] if first else [dx_acc]))
            return out[:3], (out[3:] if last else out[3])

        x_rows = pack(x_recv, "pack_x")
        a0, b0, acc = forward(q_own, None, True, False)
        a1, b1, acc = forward(q_twin, acc, False, False)
        a2, b2, acc = forward(q_split, acc, False, False)
        a3, b3, y_send = forward(q_far, acc, False, True)
        y_recv = [y_send[0]] + [lax.ppermute(y_send[s], dev_axes, back[s]) for s in range(1, N_SHIFT)]

        c_rows = pack(c_recv, "pack_c")
        g_far, acc = backward(q_far, (a3, b3), None, True, False)
        g_far = permute(g_far, twin_pairs)
        g_split, acc = backward(q_split, (a2, b2), acc, False, False)
        g_twin, acc = backward(q_twin, (a1, b1), acc, False, False)
        g_twin = permute(g_twin, twin_pairs)
        g_split = permute([a + b for a, b in zip(g_split, g_far)], split_pairs)
        g_own, dx_send = backward(q_own, (a0, b0), acc, False, True)
        dx_recv = [dx_send[0]] + [lax.ppermute(dx_send[s], dev_axes, back[s]) for s in range(1, N_SHIFT)]

        route_frac = total_count.astype(F32) / (2 * n_tokens)
        aux_weight = (AUX_COEF * n_experts / n_tokens) * route_frac
        weight_row = jnp.concatenate([jnp.tile(aux_weight, 6), jnp.zeros((128 - 6 * n_experts,), F32)])[None, :]

        def tok_block(w):
            return pl.BlockSpec((TOK_TILE, w), lambda t: (t, 0))

        def whole(shape):
            return pl.BlockSpec(shape, lambda t: (0, 0))

        combine_scratch = [slot_buf, pltpu.VMEM((n_experts * WIN, d_model), BF16), dma8]
        output, dz, dwr = pl.pallas_call(
            y_combine_kernel, grid=(tok_rows // TOK_TILE,),
            in_specs=[smem()] * 3 + [hbm()] * N_SHIFT + [tok_block(128), tok_block(d_model), tok_block(d_model), whole((1, 128))],
            out_specs=[tok_block(d_model), tok_block(128), whole((128, d_model))],
            out_shape=[jax.ShapeDtypeStruct((tok_rows, d_model), BF16), jax.ShapeDtypeStruct((tok_rows, 128), BF16), jax.ShapeDtypeStruct((128, d_model), F32)],
            scratch_shapes=combine_scratch,
            compiler_params=params("arbitrary"), cost_estimate=cost(2 * spread_flops, 4 * rows * d_model), name="y_combine",
        )(order, base, my_kept, *y_recv, info, hidden, d_out, weight_row)
        dwr_t = dwr[0:n_experts] + dwr[2 * n_experts:3 * n_experts] + dwr[5 * n_experts:6 * n_experts]
        dwr_t, prob_total = lax.psum((dwr_t, prob_sum[:, 0]), all_axes)
        d_router = dwr_t.T
        aux_loss = AUX_COEF * n_experts * jnp.sum(route_frac * (prob_total / n_tokens))

        d_hidden = pl.pallas_call(
            dx_combine_kernel, grid=(tok_rows // TOK_TILE,),
            in_specs=[smem()] * 3 + [hbm()] * N_SHIFT + [tok_block(128), tok_block(128), tok_block(d_model), whole((128, d_model))],
            out_specs=tok_block(d_model),
            out_shape=jax.ShapeDtypeStruct((tok_rows, d_model), BF16),
            scratch_shapes=combine_scratch,
            compiler_params=params("arbitrary"), cost_estimate=cost(spread_flops, 4 * rows * d_model), name="dx_combine",
        )(order, base, my_kept, *dx_recv, info, dz, d_out, wr6)

        def finish(own, got, other):
            r, w = own.shape
            tile = r // 4
            spec = pl.BlockSpec((tile, w), lambda e, i, j: (i, 0))
            return pl.pallas_call(
                finish_kernel,
                grid_spec=pltpu.PrefetchScalarGridSpec(
                    num_scalar_prefetch=1, grid=(2, 4),
                    in_specs=[spec] * 3, out_specs=pl.BlockSpec((1, tile, w), lambda e, i, j: (e, i, 0))),
                out_shape=jax.ShapeDtypeStruct((2, r, w), F32),
                compiler_params=params("arbitrary", "arbitrary"), cost_estimate=cost(10**9, 24 * r * w), name="finish",
            )(mine[None].astype(I32), own, got, other)

        d_gate, d_up, d_down = [finish(own, got, other) for own, got, other in zip(g_own, g_twin, g_split)]
        return output, d_hidden, d_router, aux_loss, d_gate, d_up, d_down

    return jax.shard_map(layer, mesh=mesh, in_specs=(tok_spec, P(), tok_spec, tok_spec, gate_spec, gate_spec, down_spec), out_specs=(tok_spec, tok_spec, P(), P(), gate_spec, gate_spec, down_spec), check_vma=False)
```

```python
import functools
import jax
import jax.numpy as jnp
from jax import lax
from jax.experimental import pallas as pl
from jax.experimental.pallas import tpu as pltpu
from jax.sharding import PartitionSpec as P


AUX_COEF = 0.01
OUT_SCALE = 2.0
BF16 = jnp.bfloat16
F32 = jnp.float32
I32 = jnp.int32
VMEM_LIMIT = 62 * 1024 * 1024


N_SHIFT = 8
TOK_TILE = 256
ROW_TILE = 512
ALIGN = 16
WIN = TOK_TILE + ALIGN


def coords(i):
    return (i >> 3) & 1, (i >> 2) & 1, (i >> 1) & 1, i & 1


def index_of(z, y, x, c):
    return (z << 3) | (y << 2) | (x << 1) | c


def shift_dest(i, s):
    z, y, x, c = coords(i)
    x, c, d = x ^ ((s >> 2) & 1), c ^ ((s >> 1) & 1), s & 1
    return index_of(z, y ^ d, x, c) if c == 0 else index_of(z ^ d, y, x, c)


def split_partner(i):
    z, y, x, c = coords(i)
    return index_of(z, y ^ 1, x, c) if c == 0 else index_of(z ^ 1, y, x, c)


def twin_partner(i):
    z, y, x, c = coords(i)
    return index_of(z ^ 1, y, x, c) if c == 0 else index_of(z, y ^ 1, x, c)


def dot_nn(a, b):
    return lax.dot_general(a, b, (((1,), (0,)), ((), ())), preferred_element_type=F32)


def dot_nt(a, b):
    return lax.dot_general(a, b, (((1,), (1,)), ((), ())), preferred_element_type=F32)


def dot_tn(a, b):
    return lax.dot_general(a, b, (((0,), (0,)), ((), ())), preferred_element_type=F32)


def iota(shape, dim):
    return lax.broadcasted_iota(I32, shape, dim)


def tile_columns(ids_t, starts, limits, n_experts, upper):
    tokens = ids_t.shape[1]
    e_iota = iota((n_experts, tokens), 0)
    hot0 = ids_t[0:1, :] == e_iota
    hot1 = ids_t[1:2, :] == e_iota
    either = jnp.where(hot0 | hot1, 1.0, 0.0).astype(BF16)
    before = dot_nn(either, upper).astype(I32)
    offset = jnp.zeros((n_experts, tokens), I32)
    bound = jnp.zeros((n_experts, tokens), I32)
    for e in range(n_experts):
        offset = jnp.where(e_iota == e, e * WIN + (starts[e] & (ALIGN - 1)), offset)
        if limits is not None:
            bound = jnp.where(e_iota == e, limits[e] - starts[e], bound)
    column = before + offset
    if limits is not None:
        column = jnp.where(before < bound, column, -1)
    return [jnp.sum(jnp.where(hot, column, 0), axis=0, keepdims=True) for hot in (hot0, hot1)]


def strict_upper(n):
    return jnp.where(iota((n, n), 0) < iota((n, n), 1), 1.0, 0.0).astype(BF16)


def add_windows(buf, value, starts, n_experts):
    for e in range(n_experts):
        rows = pl.ds(pl.multiple_of(starts[e] - (starts[e] & (ALIGN - 1)), ALIGN), WIN)
        buf[e, rows, :] = buf[e, rows, :] + value[e * WIN:(e + 1) * WIN, :]


def slots_out(buf, order_ref, outs, sem):
    slots = outs[0].shape[0]
    copies = [pltpu.make_async_copy(buf.at[order_ref[s], pl.ds(0, slots), :], outs[s], sem.at[s]) for s in range(N_SHIFT)]
    for copy in copies:
        copy.start()
    for copy in copies:
        copy.wait()


def counts_kernel(n_dev, etp_size, ids_ref, table_ref, mine_ref, send_sem, recv_sem):
    etp, ep = lax.axis_index("etp"), lax.axis_index("ep")
    ep_size = n_dev // etp_size
    me = ep * etp_size + etp
    tokens = ids_ref.shape[1]
    e_iota = iota((128, tokens), 0)
    hot = (ids_ref[0:1, :] == e_iota) | (ids_ref[1:2, :] == e_iota)
    counts = dot_nt(jnp.ones((8, tokens), BF16), jnp.where(hot, 1.0, 0.0).astype(BF16)).astype(I32)
    mine_ref[...] = counts
    table_ref[me] = counts

    def peer(k):
        return {"ep": lax.rem(ep + k // etp_size, ep_size), "etp": lax.rem(etp + k % etp_size, etp_size)}

    barrier = pltpu.get_barrier_semaphore()
    for k in range(1, n_dev):
        pl.semaphore_signal(barrier, inc=1, device_id=peer(k), device_id_type=pl.DeviceIdType.MESH)
    pl.semaphore_wait(barrier, n_dev - 1)
    copies = [pltpu.make_async_remote_copy(
        src_ref=mine_ref, dst_ref=table_ref.at[me], send_sem=send_sem.at[k], recv_sem=recv_sem.at[k],
        device_id=peer(k), device_id_type=pl.DeviceIdType.MESH) for k in range(1, n_dev)]
    for copy in copies:
        copy.start()
    for copy in copies:
        copy.wait()


def x_slots_kernel(order_ref, ids_ref, h_ref, base_ref, *rest):
    outs, (buf, base_s, sem, base_sem) = rest[:N_SHIFT], rest[N_SHIFT:]
    n_experts, tokens = base_ref.shape[0], ids_ref.shape[1]
    e_iota = iota((n_experts, tokens), 0)
    hot = (ids_ref[0:1, :] == e_iota) | (ids_ref[1:2, :] == e_iota)
    earlier = jnp.where(iota((tokens, 128), 0) < TOK_TILE * iota((tokens, 128), 1), 1.0, 0.0).astype(BF16)
    base_ref[...] = dot_nn(jnp.where(hot, 1.0, 0.0).astype(BF16), earlier).astype(I32)
    copy = pltpu.make_async_copy(base_ref, base_s, base_sem)
    copy.start()
    buf[...] = jnp.zeros_like(buf)
    copy.wait()
    upper = strict_upper(TOK_TILE)

    @pl.loop(0, tokens // TOK_TILE)
    def _(t):
        here = pl.ds(pl.multiple_of(t * TOK_TILE, TOK_TILE), TOK_TILE)
        starts = [base_s[e, t] for e in range(n_experts)]
        col0, col1 = tile_columns(ids_ref[:, here], starts, None, n_experts, upper)
        row = iota((n_experts * WIN, TOK_TILE), 0)
        pick = jnp.where((row == col0) | (row == col1), 1.0, 0.0).astype(BF16)
        add_windows(buf, dot_nn(pick, h_ref[here, :]).astype(BF16), starts, n_experts)

    slots_out(buf, order_ref, outs, sem)


def c_slots_kernel(order_ref, base_s, limit_s, ids_ref, h_ref, dy_ref, wr3_ref, info_ref, psum_ref, *rest):
    outs, (buf, prob_buf, sem) = rest[:N_SHIFT], rest[N_SHIFT:]
    n_experts, tokens = psum_ref.shape[0], ids_ref.shape[1]
    parts = dot_nt(wr3_ref[...], h_ref[...])
    logits = parts[2 * n_experts:3 * n_experts] + parts[n_experts:2 * n_experts] + parts[0:n_experts]
    top = jnp.max(logits, axis=0, keepdims=True)
    expo = jnp.exp(logits - top)
    prob = expo / jnp.sum(expo, axis=0, keepdims=True)
    prob_buf[...] = prob
    psum_ref[...] = jnp.broadcast_to(jnp.sum(prob, axis=1, keepdims=True), psum_ref.shape)
    buf[...] = jnp.zeros_like(buf)
    upper = strict_upper(TOK_TILE)
    limits = [limit_s[e] for e in range(n_experts)]

    @pl.loop(0, tokens // TOK_TILE)
    def _(t):
        here = pl.ds(pl.multiple_of(t * TOK_TILE, TOK_TILE), TOK_TILE)
        starts = [base_s[e, t] for e in range(n_experts)]
        ids_t = ids_ref[:, here]
        p_t = prob_buf[:, here]
        e_iota = iota((n_experts, TOK_TILE), 0)
        p0 = jnp.sum(jnp.where(ids_t[0:1, :] == e_iota, p_t, 0.0), axis=0, keepdims=True)
        p1 = jnp.sum(jnp.where(ids_t[1:2, :] == e_iota, p_t, 0.0), axis=0, keepdims=True)
        total = p0 + p1
        g0, g1 = p0 / total, p1 / total
        col0, col1 = tile_columns(ids_t, starts, limits, n_experts, upper)
        row = iota((n_experts * WIN, TOK_TILE), 0)
        is0, is1 = row == col0, row == col1
        pick = jnp.where(is0 | is1, 1.0, 0.0).astype(BF16)
        gate = jnp.sum(jnp.where(is0, g0, jnp.where(is1, g1, 0.0)), axis=1, keepdims=True)
        mixed = OUT_SCALE * dot_nn(pick, dy_ref[here, :])
        add_windows(buf, (gate * mixed).astype(BF16), starts, n_experts)
        group = iota((8, TOK_TILE), 0)
        extra = jnp.zeros((8, TOK_TILE), F32)
        for k, v in enumerate((g0, g1, col0.astype(F32), col1.astype(F32), ids_t[0:1, :].astype(F32), ids_t[1:2, :].astype(F32))):
            extra = jnp.where(group == k, v, extra)
        table = jnp.concatenate([p_t] * 6 + [extra, jnp.zeros((128 - 6 * n_experts - 8, TOK_TILE), F32)], axis=0)
        info_ref[here, :] = table.T

    slots_out(buf, order_ref, outs, sem)


def pack_kernel(count_s, offset_s, *refs):
    ins, out_ref, (buf, sem, out_sem) = refs[:N_SHIFT], refs[N_SHIFT], refs[N_SHIFT + 1:]
    sizes = [512, 256, 128, 64, 32, 16]

    def for_parts(act):
        for s in range(N_SHIFT):
            count, offset = count_s[s], offset_s[s]
            done = jnp.int32(0)
            for j, size in enumerate(sizes):
                has = (count & size) != 0
                start = pl.multiple_of(done, ALIGN)
                dest = pl.multiple_of(offset + done, ALIGN)

                @pl.when(has)
                def _(s=s, j=j, size=size, start=start, dest=dest):
                    act(pltpu.make_async_copy(ins[s].at[pl.ds(start, size), :], buf.at[pl.ds(dest, size), :], sem.at[s, j]))

                done = done + jnp.where(has, size, 0)

    for_parts(lambda copy: copy.start())
    total = pl.multiple_of(offset_s[N_SHIFT], ALIGN)
    buf[pl.ds(total, ROW_TILE), :] = jnp.zeros((ROW_TILE, buf.shape[1]), buf.dtype)
    for_parts(lambda copy: copy.wait())
    copy = pltpu.make_async_copy(buf.at[pl.ds(0, out_ref.shape[0]), :], out_ref, out_sem)
    copy.start()
    copy.wait()


def rows_out(buf, offset_s, outs, sem):
    slots = outs[0].shape[0]
    copies = [pltpu.make_async_copy(buf.at[pl.ds(pl.multiple_of(offset_s[s], ALIGN), slots), :], outs[s], sem.at[s]) for s in range(N_SHIFT)]
    for copy in copies:
        copy.start()
    for copy in copies:
        copy.wait()


def forward_kernel(n_ref, offset_s, x_ref, w1_ref, w3_ref, w2_ref, *rest, first, last):
    rest = list(rest)
    y_in = None if first else rest.pop(0)
    a_ref, b_ref = rest.pop(0), rest.pop(0)
    if last:
        outs, (buf, sem) = rest[:N_SHIFT], rest[N_SHIFT:]
    else:
        (y_out,) = rest
    i = pl.program_id(0)

    @pl.when(i < n_ref[0])
    def _():
        a = dot_nn(x_ref[...], w1_ref[...])
        b = dot_nn(x_ref[...], w3_ref[...])
        a_ref[...] = a
        b_ref[...] = b
        y = dot_nn((a * jax.nn.sigmoid(a) * b).astype(BF16), w2_ref[...])
        if not first:
            y = y_in[...] + y
        if last:
            buf[pl.ds(pl.multiple_of(i * ROW_TILE, ROW_TILE), ROW_TILE), :] = y.astype(BF16)
        else:
            y_out[...] = y

    if last:
        @pl.when(i == pl.num_programs(0) - 1)
        def _():
            rows_out(buf, offset_s, outs, sem)


def clear(refs):
    @pl.when(pl.program_id(0) == 0)
    def _():
        for ref in refs:
            ref[...] = jnp.zeros_like(ref)


def act_grads(c_ref, a_ref, b_ref, w2_ref):
    du = dot_nt(c_ref[...], w2_ref[...])
    a, b = a_ref[...], b_ref[...]
    sig = jax.nn.sigmoid(a)
    silu = a * sig
    da = (du * b * sig * (1.0 + a * (1.0 - sig))).astype(BF16)
    return da, (du * silu).astype(BF16), (silu * b).astype(BF16)


def add_weight_grads(x, c, da, db, u, g1_ref, g3_ref, g2_ref):
    g1_ref[...] += dot_tn(x, da)
    g3_ref[...] += dot_tn(x, db)
    g2_ref[...] += dot_tn(u, c)


def backward_kernel(n_ref, offset_s, x_ref, c_ref, a_ref, b_ref, w1_ref, w3_ref, w2_ref, *rest, first):
    dx_in = None if first else rest[0]
    g1_ref, g3_ref, g2_ref, dx_out = rest[-4:]
    clear((g1_ref, g3_ref, g2_ref))

    @pl.when(pl.program_id(0) < n_ref[0])
    def _():
        da, db, u = act_grads(c_ref, a_ref, b_ref, w2_ref)
        dx = dot_nt(da, w1_ref[...]) + dot_nt(db, w3_ref[...])
        dx_out[...] = dx if first else dx_in[...] + dx
        add_weight_grads(x_ref[...], c_ref[...], da, db, u, g1_ref, g3_ref, g2_ref)


def backward_rows_kernel(n_ref, offset_s, c_ref, a_ref, b_ref, w1_ref, w3_ref, w2_ref, dx_in, da_ref, db_ref, u_ref, *rest):
    outs, (buf, sem) = rest[:N_SHIFT], rest[N_SHIFT:]
    i = pl.program_id(0)

    @pl.when(i < n_ref[0])
    def _():
        da, db, u = act_grads(c_ref, a_ref, b_ref, w2_ref)
        da_ref[...] = da
        db_ref[...] = db
        u_ref[...] = u
        dx = dx_in[...] + (dot_nt(da, w1_ref[...]) + dot_nt(db, w3_ref[...]))
        buf[pl.ds(pl.multiple_of(i * ROW_TILE, ROW_TILE), ROW_TILE), :] = dx.astype(BF16)

    @pl.when(i == pl.num_programs(0) - 1)
    def _():
        rows_out(buf, offset_s, outs, sem)


def weight_grads_kernel(n_ref, offset_s, x_ref, c_ref, da_ref, db_ref, u_ref, g1_ref, g3_ref, g2_ref):
    clear((g1_ref, g3_ref, g2_ref))

    @pl.when(pl.program_id(0) < n_ref[0])
    def _():
        add_weight_grads(x_ref[...], c_ref[...], da_ref[...], db_ref[...], u_ref[...], g1_ref, g3_ref, g2_ref)


def load_slots(order_ref, ins, buf, sem):
    slots = ins[0].shape[0]
    copies = [pltpu.make_async_copy(ins[s], buf.at[order_ref[s], pl.ds(0, slots), :], sem.at[s]) for s in range(N_SHIFT)]
    for copy in copies:
        copy.start()
    for copy in copies:
        copy.wait()


def gather_windows(buf, window, base_s, kept_s, t, n_experts):
    for e in range(n_experts):
        start = base_s[e, t] - (base_s[e, t] & (ALIGN - 1))
        rows = buf[e, pl.ds(pl.multiple_of(start, ALIGN), WIN), :]
        valid = iota(rows.shape, 0) < kept_s[e] - start
        window[e * WIN:(e + 1) * WIN, :] = jnp.where(valid, rows, jnp.zeros_like(rows))


def y_combine_kernel(order_ref, base_s, kept_s, *refs):
    ins, refs = refs[:N_SHIFT], refs[N_SHIFT:]
    info_ref, h_ref, dy_ref, w_ref, out_ref, dz_ref, dwr_ref, buf, window, sem = refs
    n_experts = buf.shape[0]
    t = pl.program_id(0)

    @pl.when(t == 0)
    def _():
        load_slots(order_ref, ins, buf, sem)
        dwr_ref[...] = jnp.zeros_like(dwr_ref)

    gather_windows(buf, window, base_s, kept_s, t, n_experts)
    info = info_ref[...]
    k0 = 6 * n_experts
    g0, g1, col0, col1, e0, e1 = [info[:, k0 + k:k0 + k + 1] for k in range(6)]
    col = iota((TOK_TILE, n_experts * WIN), 1)
    pick0 = jnp.where(col == col0.astype(I32), 1.0, 0.0).astype(BF16)
    pick1 = jnp.where(col == col1.astype(I32), 1.0, 0.0).astype(BF16)
    y0 = dot_nn(pick0, window[...])
    y1 = dot_nn(pick1, window[...])
    h = h_ref[...]
    mix = OUT_SCALE * dy_ref[...].astype(F32)
    out_ref[...] = (h.astype(F32) + OUT_SCALE * (g0 * y0 + g1 * y1)).astype(BF16)
    dg0 = jnp.sum(mix * y0, axis=1, keepdims=True)
    dg1 = jnp.sum(mix * y1, axis=1, keepdims=True)
    lane = iota(info.shape, 1)
    prob = jnp.where(lane < k0, info, 0.0)
    weight = w_ref[...]
    mean_w = jnp.sum(jnp.where(lane < n_experts, prob * weight, 0.0), axis=1, keepdims=True)
    expert = (lane & (n_experts - 1)).astype(F32)
    sign = jnp.where(expert == e0, 1.0, 0.0) - jnp.where(expert == e1, 1.0, 0.0)
    dz = prob * (weight - mean_w) + g0 * g1 * (dg0 - dg1) * jnp.where(lane < k0, sign, 0.0)
    d1 = dz.astype(BF16)
    rem1 = dz - d1.astype(F32)
    d2 = rem1.astype(BF16)
    d3 = (rem1 - d2.astype(F32)).astype(BF16)
    group = lane // n_experts
    first = (group == 0) | (group == 1) | (group == 3)
    second = (group == 2) | (group == 4)
    dzp = jnp.where(first, d1.astype(F32), jnp.where(second, d2.astype(F32), d3.astype(F32))).astype(BF16)
    dz_ref[...] = dzp
    dwr_ref[...] += dot_tn(dzp, h)


def dx_combine_kernel(order_ref, base_s, kept_s, *refs):
    ins, refs = refs[:N_SHIFT], refs[N_SHIFT:]
    info_ref, dz_ref, dy_ref, wr_ref, out_ref, buf, window, sem = refs
    n_experts = buf.shape[0]
    t = pl.program_id(0)

    @pl.when(t == 0)
    def _():
        load_slots(order_ref, ins, buf, sem)

    gather_windows(buf, window, base_s, kept_s, t, n_experts)
    info = info_ref[...]
    k0 = 6 * n_experts
    col0, col1 = info[:, k0 + 2:k0 + 3].astype(I32), info[:, k0 + 3:k0 + 4].astype(I32)
    col = iota((TOK_TILE, n_experts * WIN), 1)
    pick = jnp.where((col == col0) | (col == col1), 1.0, 0.0).astype(BF16)
    total = dy_ref[...].astype(F32) + dot_nn(pick, window[...]) + dot_nn(dz_ref[...], wr_ref[...])
    out_ref[...] = total.astype(BF16)


def finish_kernel(j_ref, own_ref, part_ref, other_ref, out_ref):
    own = pl.program_id(0) == 0

    @pl.when(own)
    def _():
        out_ref[0] = own_ref[...] + part_ref[...]

    @pl.when(jnp.logical_not(own))
    def _():
        out_ref[0] = other_ref[...]


def params(*semantics):
    return pltpu.CompilerParams(dimension_semantics=semantics or None, vmem_limit_bytes=VMEM_LIMIT)


def hbm():
    return pl.BlockSpec(memory_space=pl.ANY)


def smem():
    return pl.BlockSpec(memory_space=pltpu.SMEM)


def vmem():
    return pl.BlockSpec(memory_space=pltpu.VMEM)


def cost(flops, nbytes):
    return pl.CostEstimate(flops=int(flops), bytes_accessed=int(nbytes), transcendentals=0)


def split3(v):
    p1 = v.astype(BF16)
    r1 = v - p1.astype(F32)
    p2 = r1.astype(BF16)
    return p1, p2, (r1 - p2.astype(F32)).astype(BF16)


def solution(mesh):
    ep_size = mesh.shape["ep"]
    etp_size = mesh.shape["etp"]
    n_dev = ep_size * etp_size
    all_axes = ("ep", "etp")
    dev_axes = ("etp", "ep")
    tok_spec = P(all_axes, None)
    gate_spec = P("ep", None, "etp")
    down_spec = P("ep", "etp", None)

    def layer(hidden, w_router, expert_ids, d_out, w_gate, w_up, w_down):
        tok_rows, d_model = hidden.shape
        n_experts = w_router.shape[1]
        n_tokens = tok_rows * n_dev
        capacity = (5 * n_tokens + 2 * n_experts - 1) // (2 * n_experts)
        slots = 7 * tok_rows // (2 * n_experts)
        width = w_gate.shape[2]
        rows = N_SHIFT * slots
        buf_rows = slots + WIN + ALIGN
        etp, ep = lax.axis_index("etp"), lax.axis_index("ep")
        z, y, x, c = etp >> 1, etp & 1, ep >> 1, ep & 1
        mine = jnp.where(c == 0, y, z)

        def permute(values, pairs):
            return [lax.ppermute(v, dev_axes, pairs) for v in values]

        def exchange(parts, pairs):
            out = [parts[0]]
            for s in range(1, N_SHIFT):
                out.append(lax.ppermute(parts[s], dev_axes, pairs[s]))
            return out

        forth = [[(i, shift_dest(i, s)) for i in range(n_dev)] for s in range(N_SHIFT)]
        back = [[(b, a) for a, b in pairs] for pairs in forth]
        split_pairs = [(i, split_partner(i)) for i in range(n_dev)]
        twin_pairs = [(i, twin_partner(i)) for i in range(n_dev)]

        order = []
        source = []
        for s in range(N_SHIFT):
            dx, dc, d = (s >> 2) & 1, (s >> 1) & 1, s & 1
            order.append(4 * (x ^ dx) + 2 * (c ^ dc) + (jnp.where((c ^ dc) == 0, y, z) ^ d))
            sx, sc = x ^ dx, c ^ dc
            sz = jnp.where(c == 0, z, z ^ d)
            sy = jnp.where(c == 0, y ^ d, y)
            source.append((sx * 2 + sc) * etp_size + sz * 2 + sy)
        order = jnp.stack(order).astype(I32)
        source = jnp.stack(source).astype(I32)

        ids_t = expert_ids.T
        slot_shape = jax.ShapeDtypeStruct((slots, d_model), BF16)
        slot_buf = pltpu.VMEM((n_experts, buf_rows, d_model), BF16)
        dma8 = pltpu.SemaphoreType.DMA((N_SHIFT,))
        spread_flops = 2 * tok_rows * n_experts * WIN * d_model

        count_table = pl.pallas_call(
            functools.partial(counts_kernel, n_dev, etp_size),
            in_specs=[vmem()], out_specs=vmem(),
            out_shape=jax.ShapeDtypeStruct((n_dev, 8, 128), I32),
            scratch_shapes=[pltpu.VMEM((8, 128), I32), pltpu.SemaphoreType.DMA((n_dev,)), pltpu.SemaphoreType.DMA((n_dev,))],
            compiler_params=pltpu.CompilerParams(collective_id=0, has_side_effects=True), name="counts",
        )(ids_t)[:, 0, :n_experts]

        x_slots = pl.pallas_call(
            x_slots_kernel,
            in_specs=[smem(), vmem(), vmem()],
            out_specs=[vmem()] + [hbm()] * N_SHIFT,
            out_shape=[jax.ShapeDtypeStruct((n_experts, 128), I32)] + [slot_shape] * N_SHIFT,
            scratch_shapes=[slot_buf, pltpu.SMEM((n_experts, 128), I32), dma8, pltpu.SemaphoreType.DMA],
            compiler_params=params(), cost_estimate=cost(spread_flops, 2 * rows * d_model), name="x_slots",
        )
        base, *x_send = x_slots(order + jnp.minimum(count_table[0, 0], 0), ids_t, hidden)
        x_recv = exchange(x_send, forth)

        running = jnp.cumsum(count_table, axis=0) - count_table
        total_count = jnp.sum(count_table, axis=0)
        block_idx = ep * etp_size + etp
        limit = jnp.clip(capacity - running, 0, None)
        kept_table = jnp.minimum(count_table, limit)
        my_limit, my_kept = limit[block_idx], kept_table[block_idx]
        my_expert = order[0]
        part = (kept_table[source, my_expert] + ALIGN - 1) // ALIGN * ALIGN
        offset = jnp.concatenate([jnp.zeros((1,), I32), jnp.cumsum(part)]).astype(I32)
        n_tiles = (offset[N_SHIFT:] + ROW_TILE - 1) // ROW_TILE

        wr_t = split3(w_router.T)
        wr3 = jnp.concatenate(wr_t + (jnp.zeros_like(wr_t[0]),), axis=0)
        wr6 = jnp.concatenate([wr_t[0], wr_t[1], wr_t[0], wr_t[2], wr_t[1], wr_t[0], jnp.zeros((128 - 6 * n_experts, d_model), BF16)], axis=0)
        c_slots = pl.pallas_call(
            c_slots_kernel,
            in_specs=[smem()] * 3 + [vmem()] * 4,
            out_specs=[vmem()] * 2 + [hbm()] * N_SHIFT,
            out_shape=[jax.ShapeDtypeStruct((tok_rows, 128), F32), jax.ShapeDtypeStruct((n_experts, 128), F32)] + [slot_shape] * N_SHIFT,
            scratch_shapes=[slot_buf, pltpu.VMEM((n_experts, tok_rows), F32), dma8],
            compiler_params=params(), cost_estimate=cost(spread_flops, 2 * rows * d_model), name="c_slots",
        )
        info, prob_sum, *c_send = c_slots(order, base, my_limit, ids_t, hidden, d_out, wr3)

        def take(w, j):
            return lax.dynamic_index_in_dim(w, j, 0, keepdims=False)

        weights = (w_gate, w_up, w_down)
        early = mine + jnp.minimum(count_table[0, 0], 0)
        later = mine + jnp.minimum(prob_sum[0, 0], 0.0).astype(I32)
        when = (later, later, early)
        q_own = [take(w, j) for w, j in zip(weights, when)]
        q_other = [take(w, 1 - j) for w, j in zip(weights, when)]
        q_split = permute(q_other[:2], split_pairs) + permute(q_other[2:], split_pairs)
        q_twin = permute(q_own[:2], twin_pairs) + permute(q_own[2:], twin_pairs)
        q_far = permute(q_split, twin_pairs)

        def after(value, earlier):
            return lax.optimization_barrier((value, earlier))[0]

        c_recv = exchange(c_send, forth)

        def pack(parts):
            return pl.pallas_call(
                pack_kernel,
                in_specs=[smem()] * 2 + [hbm()] * N_SHIFT,
                out_specs=hbm(),
                out_shape=jax.ShapeDtypeStruct((rows, d_model), BF16),
                scratch_shapes=[pltpu.VMEM((rows + ROW_TILE, d_model), BF16), pltpu.SemaphoreType.DMA((N_SHIFT, 6)), pltpu.SemaphoreType.DMA],
                compiler_params=params(), cost_estimate=cost(10**9, 4 * rows * d_model),
            )(part, offset, *parts)

        def row_spec(w):
            return pl.BlockSpec((ROW_TILE, w), lambda i, n, o: (jnp.clip(n[0] - 1, 0, i), 0))

        def full_spec(shape):
            return pl.BlockSpec(shape, lambda i, n, o: (0, 0), pipeline_mode=pl.Buffered(1))

        grid = (rows // ROW_TILE,)
        up_shape, down_shape = (d_model, width), (width, d_model)
        row_f32 = jax.ShapeDtypeStruct((rows, d_model), F32)
        act_shape = jax.ShapeDtypeStruct((rows, width), F32)
        row_buf = pltpu.VMEM((rows + slots, d_model), BF16)
        mm = 2 * rows * d_model * width

        def forward(quarter, y_acc, first, last):
            n_in = 4 + (not first)
            out = pl.pallas_call(
                functools.partial(forward_kernel, first=first, last=last),
                grid_spec=pltpu.PrefetchScalarGridSpec(
                    num_scalar_prefetch=2, grid=grid,
                    in_specs=[row_spec(d_model), full_spec(up_shape), full_spec(up_shape), full_spec(down_shape)] + [row_spec(d_model)] * (not first),
                    out_specs=[row_spec(width)] * 2 + ([hbm()] * N_SHIFT if last else [row_spec(d_model)]),
                    scratch_shapes=[row_buf, dma8] if last else []),
                out_shape=[act_shape] * 2 + ([slot_shape] * N_SHIFT if last else [row_f32]),
                input_output_aliases={} if first or last else {2 + n_in - 1: 2},
                compiler_params=params("arbitrary"), cost_estimate=cost(3 * mm, 20 * rows * d_model), name="forward",
            )(n_tiles, offset, x_rows, *quarter, *([] if first else [y_acc]))
            return out[0], out[1], (out[2:] if last else out[2])

        grad_shapes = [jax.ShapeDtypeStruct(up_shape, F32)] * 2 + [jax.ShapeDtypeStruct(down_shape, F32)]
        grad_specs = [full_spec(up_shape), full_spec(up_shape), full_spec(down_shape)]

        def backward(quarter, acts, dx_acc):
            first = dx_acc is None
            out = pl.pallas_call(
                functools.partial(backward_kernel, first=first),
                grid_spec=pltpu.PrefetchScalarGridSpec(
                    num_scalar_prefetch=2, grid=grid,
                    in_specs=[row_spec(d_model)] * 2 + [row_spec(width)] * 2 + grad_specs + [row_spec(d_model)] * (not first),
                    out_specs=grad_specs + [row_spec(d_model)]),
                out_shape=grad_shapes + [row_f32],
                input_output_aliases={} if first else {9: 3},
                compiler_params=params("arbitrary"), cost_estimate=cost(6 * mm, 20 * rows * d_model), name="backward",
            )(n_tiles, offset, x_rows, c_rows, *acts, *quarter, *([] if first else [dx_acc]))
            return out[:3], out[3]

        def backward_rows(quarter, acts, dx_acc):
            out = pl.pallas_call(
                backward_rows_kernel,
                grid_spec=pltpu.PrefetchScalarGridSpec(
                    num_scalar_prefetch=2, grid=grid,
                    in_specs=[row_spec(d_model)] + [row_spec(width)] * 2 + grad_specs + [row_spec(d_model)],
                    out_specs=[row_spec(width)] * 3 + [hbm()] * N_SHIFT,
                    scratch_shapes=[row_buf, dma8]),
                out_shape=[jax.ShapeDtypeStruct((rows, width), BF16)] * 3 + [slot_shape] * N_SHIFT,
                compiler_params=params("arbitrary"), cost_estimate=cost(3 * mm, 20 * rows * d_model), name="backward_rows",
            )(n_tiles, offset, c_rows, *acts, *quarter, dx_acc)
            return out[:3], out[3:]

        def weight_grads(grads):
            return pl.pallas_call(
                weight_grads_kernel,
                grid_spec=pltpu.PrefetchScalarGridSpec(
                    num_scalar_prefetch=2, grid=grid,
                    in_specs=[row_spec(d_model)] * 2 + [row_spec(width)] * 3,
                    out_specs=grad_specs),
                out_shape=grad_shapes,
                compiler_params=params("arbitrary"), cost_estimate=cost(3 * mm, 20 * rows * d_model), name="weight_grads",
            )(n_tiles, offset, x_rows, c_rows, *grads)

        x_rows = pack(x_recv)
        a0, b0, acc = forward(q_own, None, True, False)
        a1, b1, acc = forward(q_twin, acc, False, False)
        a2, b2, acc = forward(q_split, acc, False, False)
        a3, b3, y_send = forward(q_far, acc, False, True)
        y_recv = exchange(y_send, back)

        c_rows = pack([after(c_recv[0], y_send[0])] + c_recv[1:])
        g_far, acc = backward(q_far, (a3, b3), None)
        g_far = permute(g_far, twin_pairs)
        g_twin, acc = backward(q_twin, (a1, b1), acc)
        g_twin = permute(g_twin, twin_pairs)
        g_split, acc = backward(q_split, (a2, b2), acc)
        g_split = permute([a + b for a, b in zip(g_split, g_far)], split_pairs)
        grads, dx_send = backward_rows(q_own, (a0, b0), acc)
        dx_recv = exchange(dx_send, back)

        route_frac = total_count.astype(F32) / (2 * n_tokens)
        aux_weight = (AUX_COEF * n_experts / n_tokens) * route_frac
        weight_row = jnp.concatenate([jnp.tile(aux_weight, 6), jnp.zeros((128 - 6 * n_experts,), F32)])[None, :]

        def tok_block(w):
            return pl.BlockSpec((TOK_TILE, w), lambda t: (t, 0))

        def whole(shape):
            return pl.BlockSpec(shape, lambda t: (0, 0))

        combine_scratch = [slot_buf, pltpu.VMEM((n_experts * WIN, d_model), BF16), dma8]
        y_combine = pl.pallas_call(
            y_combine_kernel, grid=(tok_rows // TOK_TILE,),
            in_specs=[smem()] * 3 + [hbm()] * N_SHIFT + [tok_block(128), tok_block(d_model), tok_block(d_model), whole((1, 128))],
            out_specs=[tok_block(d_model), tok_block(128), whole((128, d_model))],
            out_shape=[jax.ShapeDtypeStruct((tok_rows, d_model), BF16), jax.ShapeDtypeStruct((tok_rows, 128), BF16), jax.ShapeDtypeStruct((128, d_model), F32)],
            scratch_shapes=combine_scratch,
            compiler_params=params("arbitrary"), cost_estimate=cost(2 * spread_flops, 4 * rows * d_model), name="y_combine",
        )
        output, dz, dwr = y_combine(order, base, my_kept, *y_recv, after(info, dx_send[0]), hidden, d_out, weight_row)
        dwr_t = dwr[0:n_experts] + dwr[2 * n_experts:3 * n_experts] + dwr[5 * n_experts:6 * n_experts]
        shared = jnp.concatenate([dwr_t, jnp.pad(prob_sum, ((0, 0), (0, d_model - 128)))], axis=0)

        def flip(value, bits):
            return lax.ppermute(value, dev_axes, [(i, i ^ bits) for i in range(n_dev)])

        shared = shared + flip(shared, 1)
        across_x = flip(shared, 2)

        def finish(own, got, other):
            r, w = own.shape
            tile = r // 4
            own_spec = pl.BlockSpec((tile, w), lambda e, i, j: (jnp.where(e == 0, i, 3), 0))
            other_spec = pl.BlockSpec((tile, w), lambda e, i, j: (jnp.where(e == 0, 0, i), 0))
            return pl.pallas_call(
                finish_kernel,
                grid_spec=pltpu.PrefetchScalarGridSpec(
                    num_scalar_prefetch=1, grid=(2, 4),
                    in_specs=[own_spec, own_spec, other_spec], out_specs=pl.BlockSpec((1, tile, w), lambda e, i, j: (e ^ j[0], i, 0))),
                out_shape=jax.ShapeDtypeStruct((2, r, w), F32),
                compiler_params=params("arbitrary", "arbitrary"), cost_estimate=cost(10**9, 24 * r * w), name="finish",
            )(mine[None].astype(I32), own, got, other)

        g_own = weight_grads([after(grads[0], dz)] + list(grads[1:]))
        d_gate, d_up, d_down = [finish(own, got, other) for own, got, other in zip(g_own, g_twin, g_split)]
        shared = shared + after(across_x, (d_gate, d_up, d_down))
        across = [flip(shared, bits) for bits in (4, 8, 12)]

        d_hidden = pl.pallas_call(
            dx_combine_kernel, grid=(tok_rows // TOK_TILE,),
            in_specs=[smem()] * 3 + [hbm()] * N_SHIFT + [tok_block(128), tok_block(128), tok_block(d_model), whole((128, d_model))],
            out_specs=tok_block(d_model),
            out_shape=jax.ShapeDtypeStruct((tok_rows, d_model), BF16),
            scratch_shapes=combine_scratch,
            compiler_params=params("arbitrary"), cost_estimate=cost(spread_flops, 4 * rows * d_model), name="dx_combine",
        )(order, base, my_kept, *dx_recv, after(info, (d_gate, d_up, d_down)), dz, d_out, wr6)

        across = [after(v, d_hidden) for v in across]
        shared = (shared + across[0]) + (across[1] + across[2])
        d_router = shared[:n_experts].T
        prob_total = shared[n_experts:, 0]
        aux_loss = AUX_COEF * n_experts * jnp.sum(route_frac * (prob_total / n_tokens))
        return output, d_hidden, d_router, aux_loss, d_gate, d_up, d_down

    return jax.shard_map(layer, mesh=mesh, in_specs=(tok_spec, P(), tok_spec, tok_spec, gate_spec, gate_spec, down_spec), out_specs=(tok_spec, tok_spec, P(), P(), gate_spec, gate_spec, down_spec), check_vma=False)
```

```python
import functools
import jax
import jax.numpy as jnp
import numpy as np
from jax import lax
from jax.experimental import pallas as pl
from jax.experimental.pallas import tpu as pltpu
from jax.sharding import PartitionSpec as P


AUX_COEF = 0.01
OUT_SCALE = 2.0
BF16 = jnp.bfloat16
F32 = jnp.float32
I32 = jnp.int32
VMEM_LIMIT = 62 * 1024 * 1024


N_SHIFT = 8
N_LOCAL = 4
TOK_TILE = 256
ROW_TILE = 512
ALIGN = 16
WIN = TOK_TILE + ALIGN


def coords(i):
    return (i >> 3) & 1, (i >> 2) & 1, (i >> 1) & 1, i & 1


def index_of(z, y, x, c):
    return (z << 3) | (y << 2) | (x << 1) | c


def shift_dest(i, s):
    z, y, x, c = coords(i)
    x, c, d = x ^ ((s >> 2) & 1), c ^ ((s >> 1) & 1), s & 1
    return index_of(z, y ^ d, x, c) if c == 0 else index_of(z ^ d, y, x, c)


def split_partner(i):
    z, y, x, c = coords(i)
    return index_of(z, y ^ 1, x, c) if c == 0 else index_of(z ^ 1, y, x, c)


def twin_partner(i):
    z, y, x, c = coords(i)
    return index_of(z ^ 1, y, x, c) if c == 0 else index_of(z, y ^ 1, x, c)


def dot_nn(a, b):
    return lax.dot_general(a, b, (((1,), (0,)), ((), ())), preferred_element_type=F32)


def dot_nt(a, b):
    return lax.dot_general(a, b, (((1,), (1,)), ((), ())), preferred_element_type=F32)


def dot_tn(a, b):
    return lax.dot_general(a, b, (((0,), (0,)), ((), ())), preferred_element_type=F32)


def val(ref):
    return ref[...]


def ones_where(condition):
    return jnp.where(condition, 1.0, 0.0).astype(BF16)


def iota(shape, dim):
    return lax.broadcasted_iota(I32, shape, dim)


def tile_columns(ids_t, starts, n_experts, upper, first=0):
    tokens = ids_t.shape[1]
    e_iota = iota((n_experts, tokens), 0) + first
    hot0 = ids_t[0:1, :] == e_iota
    hot1 = ids_t[1:2, :] == e_iota
    either = ones_where(hot0 | hot1)
    before = dot_nn(either, upper).astype(I32)
    offset = jnp.zeros((n_experts, tokens), I32)
    for e in range(n_experts):
        offset = jnp.where(e_iota == first + e, e * WIN + (starts[e] & (ALIGN - 1)), offset)
    column = before + offset + 1
    return [jnp.sum(jnp.where(hot, column, 0), axis=0, keepdims=True) - 1 for hot in (hot0, hot1)]


def strict_upper(n):
    return ones_where(iota((n, n), 0) < iota((n, n), 1))


def add_windows(buf, value, starts, n_experts):
    for e in range(n_experts):
        rows = pl.ds(pl.multiple_of(starts[e] - (starts[e] & (ALIGN - 1)), ALIGN), WIN)
        buf[e, rows, :] = buf[e, rows, :] + value[e * WIN:(e + 1) * WIN, :]


def slots_out(buf, order_ref, outs, sem, first=0):
    slots = outs[0].shape[0]
    copies = [pltpu.make_async_copy(buf.at[order_ref[s] - first, pl.ds(0, slots), :], out, sem.at[s]) for s, out in enumerate(outs)]
    for copy in copies:
        copy.start()
    for copy in copies:
        copy.wait()


def count_kernel(ids_ref, out_ref):
    tokens = ids_ref.shape[1]
    e_iota = iota((128, tokens), 0)
    hot = (ids_ref[0:1, :] == e_iota) | (ids_ref[1:2, :] == e_iota)
    out_ref[...] = dot_nt(jnp.ones((8, tokens), BF16), ones_where(hot)).astype(I32)


def x_slots_kernel(order_ref, ids_ref, h_ref, base_ref, *rest):
    outs, (buf, base_s, sem, base_sem) = rest[:N_LOCAL], rest[N_LOCAL:]
    n_experts, tokens = base_ref.shape[0], ids_ref.shape[1]
    lowest = order_ref[N_LOCAL]
    e_iota = iota((n_experts, tokens), 0)
    hot = (ids_ref[0:1, :] == e_iota) | (ids_ref[1:2, :] == e_iota)
    earlier = ones_where(iota((tokens, 128), 0) < TOK_TILE * iota((tokens, 128), 1))
    base_ref[...] = dot_nn(ones_where(hot), earlier).astype(I32)
    copy = pltpu.make_async_copy(base_ref, base_s, base_sem)
    copy.start()
    buf[...] = jnp.zeros_like(buf)
    copy.wait()
    upper = strict_upper(TOK_TILE)

    @pl.loop(0, tokens // TOK_TILE)
    def _(t):
        here = pl.ds(pl.multiple_of(t * TOK_TILE, TOK_TILE), TOK_TILE)
        starts = [base_s[lowest + e, t] for e in range(N_LOCAL)]
        col0, col1 = tile_columns(ids_ref[:, here], starts, N_LOCAL, upper, lowest)
        row = iota((N_LOCAL * WIN, TOK_TILE), 0)
        pick = ones_where((row == col0) | (row == col1))
        add_windows(buf, dot_nn(pick, h_ref[here, :]).astype(BF16), starts, N_LOCAL)

    slots_out(buf, order_ref, outs, sem, lowest)


def c_slots_kernel(order_ref, base_s, ids_ref, h_ref, dy_ref, wr3_ref, info_ref, psum_ref, *rest):
    outs, (buf, prob_buf, sem) = rest[:N_SHIFT], rest[N_SHIFT:]
    n_experts, tokens = psum_ref.shape[0], ids_ref.shape[1]
    parts = dot_nt(val(wr3_ref), val(h_ref))
    logits = parts[2 * n_experts:3 * n_experts] + parts[n_experts:2 * n_experts] + parts[0:n_experts]
    top = jnp.max(logits, axis=0, keepdims=True)
    expo = jnp.exp(logits - top)
    prob = expo / jnp.sum(expo, axis=0, keepdims=True)
    prob_buf[...] = prob
    psum_ref[...] = jnp.broadcast_to(jnp.sum(prob, axis=1, keepdims=True), psum_ref.shape)
    buf[...] = jnp.zeros_like(buf)
    upper = strict_upper(TOK_TILE)

    @pl.loop(0, tokens // TOK_TILE)
    def _(t):
        here = pl.ds(pl.multiple_of(t * TOK_TILE, TOK_TILE), TOK_TILE)
        starts = [base_s[e, t] for e in range(n_experts)]
        ids_t = ids_ref[:, here]
        p_t = prob_buf[:, here]
        e_iota = iota((n_experts, TOK_TILE), 0)
        p0 = jnp.sum(jnp.where(ids_t[0:1, :] == e_iota, p_t, 0.0), axis=0, keepdims=True)
        p1 = jnp.sum(jnp.where(ids_t[1:2, :] == e_iota, p_t, 0.0), axis=0, keepdims=True)
        total = p0 + p1
        g0, g1 = p0 / total, p1 / total
        col0, col1 = tile_columns(ids_t, starts, n_experts, upper)
        row = iota((n_experts * WIN, TOK_TILE), 0)
        is0, is1 = row == col0, row == col1
        pick = ones_where(is0 | is1)
        gate = jnp.sum(jnp.where(is0, g0, jnp.where(is1, g1, 0.0)), axis=1, keepdims=True)
        mixed = OUT_SCALE * dot_nn(pick, dy_ref[here, :])
        add_windows(buf, (gate * mixed).astype(BF16), starts, n_experts)
        group = iota((8, TOK_TILE), 0)
        extra = jnp.zeros((8, TOK_TILE), F32)
        for k, v in enumerate((g0, g1, col0.astype(F32), col1.astype(F32), ids_t[0:1, :].astype(F32), ids_t[1:2, :].astype(F32))):
            extra = jnp.where(group == k, v, extra)
        table = jnp.concatenate([p_t] * 6 + [extra, jnp.zeros((128 - 6 * n_experts - 8, TOK_TILE), F32)], axis=0)
        info_ref[here, :] = table.T

    slots_out(buf, order_ref, outs, sem)


def pack_rows(kept_s, offset_s, ins, out_ref, buf, sem, out_sem):
    sizes = [512, 256, 128, 64, 32, 16]

    def for_parts(s, act):
        offset = offset_s[s]
        count = offset_s[s + 1] - offset
        done = jnp.int32(0)
        for j, size in enumerate(sizes):
            has = (count & size) != 0
            start = pl.multiple_of(done, ALIGN)
            dest = pl.multiple_of(offset + done, ALIGN)

            @pl.when(has)
            def _(j=j, size=size, start=start, dest=dest):
                rows = pl.ds(dest, size)
                act(lambda: pltpu.make_async_copy(ins[s].at[pl.ds(start, size), :], buf.at[rows, :], sem.at[s, j]),
                    lambda: pltpu.make_async_copy(buf.at[rows, :], out_ref.at[rows, :], out_sem.at[s, j]))

            done = done + jnp.where(has, size, 0)

    def tail_copy():
        tail = pl.ds(pl.multiple_of(offset_s[N_SHIFT], ALIGN), ROW_TILE)
        return tail, pltpu.make_async_copy(buf.at[tail, :], out_ref.at[tail, :], out_sem.at[N_SHIFT, 0])

    def begin():
        for s in range(N_SHIFT):
            for_parts(s, lambda load, store: load().start())
        tail, copy = tail_copy()
        buf[tail, :] = jnp.zeros((ROW_TILE, buf.shape[1]), buf.dtype)
        for s in range(N_SHIFT):
            for_parts(s, lambda load, store: load().wait())
            extra = kept_s[s] & (ALIGN - 1)

            @pl.when(extra != 0)
            def _(s=s, extra=extra):
                group = pl.ds(pl.multiple_of(offset_s[s] + kept_s[s] - extra, ALIGN), ALIGN)
                rows = buf[group, :]
                buf[group, :] = jnp.where(iota(rows.shape, 0) < extra, rows, jnp.zeros_like(rows))

            for_parts(s, lambda load, store: store().start())
        copy.start()

    def end():
        for s in range(N_SHIFT):
            for_parts(s, lambda load, store: store().wait())
        tail_copy()[1].wait()

    pl.when(pl.program_id(0) == 0)(begin)
    return lambda: pl.when(pl.program_id(0) == pl.num_programs(0) - 1)(end)


def rows_out(buf, offset_s, outs, sem):
    slots = outs[0].shape[0]
    copies = [pltpu.make_async_copy(buf.at[pl.ds(pl.multiple_of(offset_s[s], ALIGN), slots), :], outs[s], sem.at[s]) for s in range(N_SHIFT)]
    for copy in copies:
        copy.start()
    for copy in copies:
        copy.wait()


def clear(refs):
    @pl.when(pl.program_id(0) == 0)
    def _():
        for ref in refs:
            ref[...] = jnp.zeros_like(ref)


def row_tile(buf):
    return buf[pl.ds(pl.multiple_of(pl.program_id(0) * ROW_TILE, ROW_TILE), ROW_TILE), :]


def forward_first_kernel(n_ref, offset_s, kept_s, *refs):
    ins, refs = refs[:N_SHIFT], refs[N_SHIFT:]
    w1_ref, w3_ref, w2_ref, a_ref, b_ref, y_out, rows_ref, buf, sem, out_sem = refs
    end = pack_rows(kept_s, offset_s, ins, rows_ref, buf, sem, out_sem)

    @pl.when(pl.program_id(0) < n_ref[0])
    def _():
        x = row_tile(buf)
        a = dot_nn(x, val(w1_ref))
        b = dot_nn(x, val(w3_ref))
        a_ref[...] = a
        b_ref[...] = b
        y_out[...] = dot_nn((a * jax.nn.sigmoid(a) * b).astype(BF16), val(w2_ref))

    end()


def forward_kernel(n_ref, offset_s, x_ref, w1_ref, w3_ref, w2_ref, y_in, a_ref, b_ref, *rest, last):
    if last:
        outs, (buf, sem) = rest[:N_SHIFT], rest[N_SHIFT:]
    i = pl.program_id(0)

    @pl.when(i < n_ref[0])
    def _():
        a = dot_nn(val(x_ref), val(w1_ref))
        b = dot_nn(val(x_ref), val(w3_ref))
        a_ref[...] = a
        b_ref[...] = b
        y = val(y_in) + dot_nn((a * jax.nn.sigmoid(a) * b).astype(BF16), val(w2_ref))
        if last:
            buf[pl.ds(pl.multiple_of(i * ROW_TILE, ROW_TILE), ROW_TILE), :] = y.astype(BF16)
        else:
            rest[0][...] = y

    if last:
        @pl.when(i == pl.num_programs(0) - 1)
        def _():
            rows_out(buf, offset_s, outs, sem)


def act_grads(du, a, b):
    sig = jax.nn.sigmoid(a)
    silu = a * sig
    da = (du * b * sig * (1.0 + a * (1.0 - sig))).astype(BF16)
    return da, (du * silu).astype(BF16), (silu * b).astype(BF16)


def add_weight_grads(x, c, da, db, u, g1_ref, g3_ref, g2_ref):
    g1_ref[...] += dot_tn(x, da)
    g3_ref[...] += dot_tn(x, db)
    g2_ref[...] += dot_tn(u, c)


def backward_first_kernel(n_ref, offset_s, kept_s, *refs):
    ins, refs = refs[:N_SHIFT], refs[N_SHIFT:]
    x_ref, a_ref, b_ref, w1_ref, w3_ref, w2_ref, g1_ref, g3_ref, g2_ref, dx_out, rows_ref, buf, sem, out_sem = refs
    clear((g1_ref, g3_ref, g2_ref))
    end = pack_rows(kept_s, offset_s, ins, rows_ref, buf, sem, out_sem)

    @pl.when(pl.program_id(0) < n_ref[0])
    def _():
        c = row_tile(buf)
        da, db, u = act_grads(dot_nt(c, val(w2_ref)), val(a_ref), val(b_ref))
        dx_out[...] = dot_nt(da, val(w1_ref)) + dot_nt(db, val(w3_ref))
        add_weight_grads(val(x_ref), c, da, db, u, g1_ref, g3_ref, g2_ref)

    end()


def backward_kernel(n_ref, offset_s, x_ref, c_ref, a_ref, b_ref, w1_ref, w3_ref, w2_ref, dx_in, g1_ref, g3_ref, g2_ref, dx_out):
    clear((g1_ref, g3_ref, g2_ref))

    @pl.when(pl.program_id(0) < n_ref[0])
    def _():
        da, db, u = act_grads(dot_nt(val(c_ref), val(w2_ref)), val(a_ref), val(b_ref))
        dx_out[...] = val(dx_in) + (dot_nt(da, val(w1_ref)) + dot_nt(db, val(w3_ref)))
        add_weight_grads(val(x_ref), val(c_ref), da, db, u, g1_ref, g3_ref, g2_ref)


def both_kernel(n_ref, offset_s, x_ref, c_ref, w1_ref, w3_ref, w2_ref, y_in, dx_in, g1_ref, g3_ref, g2_ref, dx_out, y_out):
    clear((g1_ref, g3_ref, g2_ref))

    @pl.when(pl.program_id(0) < n_ref[0])
    def _():
        x, c = val(x_ref), val(c_ref)
        a = dot_nn(x, val(w1_ref))
        b = dot_nn(x, val(w3_ref))
        da, db, u = act_grads(dot_nt(c, val(w2_ref)), a, b)
        y_out[...] = val(y_in) + dot_nn(u, val(w2_ref))
        dx_out[...] = val(dx_in) + (dot_nt(da, val(w1_ref)) + dot_nt(db, val(w3_ref)))
        add_weight_grads(x, c, da, db, u, g1_ref, g3_ref, g2_ref)


def backward_rows_kernel(n_ref, offset_s, c_ref, a_ref, b_ref, w1_ref, w3_ref, w2_ref, dx_in, *rest):
    outs, (buf, sem) = rest[:N_SHIFT], rest[N_SHIFT:]
    i = pl.program_id(0)

    @pl.when(i < n_ref[0])
    def _():
        da, db, _ = act_grads(dot_nt(val(c_ref), val(w2_ref)), val(a_ref), val(b_ref))
        dx = val(dx_in) + (dot_nt(da, val(w1_ref)) + dot_nt(db, val(w3_ref)))
        buf[pl.ds(pl.multiple_of(i * ROW_TILE, ROW_TILE), ROW_TILE), :] = dx.astype(BF16)

    @pl.when(i == pl.num_programs(0) - 1)
    def _():
        rows_out(buf, offset_s, outs, sem)


def weight_grads_kernel(n_ref, offset_s, x_ref, c_ref, a_ref, b_ref, w2_ref, g1_ref, g3_ref, g2_ref):
    clear((g1_ref, g3_ref, g2_ref))

    @pl.when(pl.program_id(0) < n_ref[0])
    def _():
        da, db, u = act_grads(dot_nt(val(c_ref), val(w2_ref)), val(a_ref), val(b_ref))
        add_weight_grads(val(x_ref), val(c_ref), da, db, u, g1_ref, g3_ref, g2_ref)


def load_slots(order_ref, ins, buf, sem):
    slots = ins[0].shape[0]
    copies = [pltpu.make_async_copy(ins[s], buf.at[order_ref[s], pl.ds(0, slots), :], sem.at[s]) for s in range(N_SHIFT)]
    for copy in copies:
        copy.start()
    for copy in copies:
        copy.wait()


def gather_windows(buf, window, base_s, kept_s, t, n_experts):
    for e in range(n_experts):
        start = base_s[e, t] - (base_s[e, t] & (ALIGN - 1))
        rows = buf[e, pl.ds(pl.multiple_of(start, ALIGN), WIN), :]
        valid = iota(rows.shape, 0) < kept_s[e] - start
        window[e * WIN:(e + 1) * WIN, :] = jnp.where(valid, rows, jnp.zeros_like(rows))


def y_combine_kernel(order_ref, base_s, kept_s, *refs):
    ins, refs = refs[:N_SHIFT], refs[N_SHIFT:]
    info_ref, h_ref, dy_ref, w_ref, out_ref, dz_ref, dwr_ref, buf, window, sem = refs
    n_experts = buf.shape[0]
    t = pl.program_id(0)

    @pl.when(t == 0)
    def _():
        load_slots(order_ref, ins, buf, sem)
        dwr_ref[...] = jnp.zeros_like(dwr_ref)

    gather_windows(buf, window, base_s, kept_s, t, n_experts)
    info = val(info_ref)
    k0 = 6 * n_experts
    g0, g1, col0, col1, e0, e1 = [info[:, k0 + k:k0 + k + 1] for k in range(6)]
    col = iota((TOK_TILE, n_experts * WIN), 1)
    pick0 = ones_where(col == col0.astype(I32))
    pick1 = ones_where(col == col1.astype(I32))
    y0 = dot_nn(pick0, val(window))
    y1 = dot_nn(pick1, val(window))
    h = val(h_ref)
    mix = OUT_SCALE * val(dy_ref).astype(F32)
    out_ref[...] = (h.astype(F32) + OUT_SCALE * (g0 * y0 + g1 * y1)).astype(BF16)
    dg0 = jnp.sum(mix * y0, axis=1, keepdims=True)
    dg1 = jnp.sum(mix * y1, axis=1, keepdims=True)
    lane = iota(info.shape, 1)
    prob = jnp.where(lane < k0, info, 0.0)
    weight = val(w_ref)
    mean_w = jnp.sum(jnp.where(lane < n_experts, prob * weight, 0.0), axis=1, keepdims=True)
    expert = (lane & (n_experts - 1)).astype(F32)
    sign = jnp.where(expert == e0, 1.0, 0.0) - jnp.where(expert == e1, 1.0, 0.0)
    dz = prob * (weight - mean_w) + g0 * g1 * (dg0 - dg1) * jnp.where(lane < k0, sign, 0.0)
    d1 = dz.astype(BF16)
    rem1 = dz - d1.astype(F32)
    d2 = rem1.astype(BF16)
    d3 = (rem1 - d2.astype(F32)).astype(BF16)
    group = lane // n_experts
    first = (group == 0) | (group == 1) | (group == 3)
    second = (group == 2) | (group == 4)
    dzp = jnp.where(first, d1.astype(F32), jnp.where(second, d2.astype(F32), d3.astype(F32))).astype(BF16)
    dz_ref[...] = dzp
    dwr_ref[...] += dot_tn(dzp, h)


def dx_combine_kernel(order_ref, base_s, kept_s, *refs):
    ins, refs = refs[:N_SHIFT], refs[N_SHIFT:]
    info_ref, dz_ref, dy_ref, wr_ref, out_ref, buf, window, sem = refs
    n_experts = buf.shape[0]
    t = pl.program_id(0)

    @pl.when(t == 0)
    def _():
        load_slots(order_ref, ins, buf, sem)

    gather_windows(buf, window, base_s, kept_s, t, n_experts)
    info = val(info_ref)
    k0 = 6 * n_experts
    col0, col1 = info[:, k0 + 2:k0 + 3].astype(I32), info[:, k0 + 3:k0 + 4].astype(I32)
    col = iota((TOK_TILE, n_experts * WIN), 1)
    pick = ones_where((col == col0) | (col == col1))
    total = val(dy_ref).astype(F32) + dot_nn(pick, val(window)) + dot_nn(val(dz_ref), val(wr_ref))
    out_ref[...] = total.astype(BF16)


def finish_own_kernel(j_ref, own_ref, part_0_ref, part_1_ref, out_ref):
    for piece, part_ref in enumerate((part_0_ref, part_1_ref)):
        @pl.when(pl.program_id(0) == piece)
        def _(part_ref=part_ref):
            out_ref[0] = val(own_ref) + val(part_ref)


def finish_other_kernel(j_ref, other_ref, _, out_ref):
    out_ref[0] = val(other_ref)


def params(*semantics):
    return pltpu.CompilerParams(dimension_semantics=semantics or None, vmem_limit_bytes=VMEM_LIMIT)


def hbm():
    return pl.BlockSpec(memory_space=pl.ANY)


def smem():
    return pl.BlockSpec(memory_space=pltpu.SMEM)


def vmem():
    return pl.BlockSpec(memory_space=pltpu.VMEM)


def cost(flops, nbytes):
    return pl.CostEstimate(flops=int(flops), bytes_accessed=int(nbytes), transcendentals=0)


def split3(v):
    p1 = v.astype(BF16)
    r1 = v - p1.astype(F32)
    p2 = r1.astype(BF16)
    return p1, p2, (r1 - p2.astype(F32)).astype(BF16)


def solution(mesh):
    ep_size = mesh.shape["ep"]
    etp_size = mesh.shape["etp"]
    n_dev = ep_size * etp_size
    all_axes = ("ep", "etp")
    dev_axes = ("etp", "ep")
    tok_spec = P(all_axes, None)
    gate_spec = P("ep", None, "etp")
    down_spec = P("ep", "etp", None)

    def layer(hidden, w_router, expert_ids, d_out, w_gate, w_up, w_down):
        tok_rows, d_model = hidden.shape
        n_experts = w_router.shape[1]
        n_tokens = tok_rows * n_dev
        capacity = (5 * n_tokens + 2 * n_experts - 1) // (2 * n_experts)
        slots = 7 * tok_rows // (2 * n_experts)
        width = w_gate.shape[2]
        rows = N_SHIFT * slots
        buf_rows = slots + WIN + ALIGN
        etp, ep = lax.axis_index("etp"), lax.axis_index("ep")
        z, y, x, c = etp >> 1, etp & 1, ep >> 1, ep & 1
        mine = jnp.where(c == 0, y, z)

        def permute(values, pairs):
            return [lax.ppermute(v, dev_axes, pairs) for v in values]

        def exchange(parts, pairs):
            out = [parts[0]]
            for s in range(1, len(parts)):
                out.append(lax.ppermute(parts[s], dev_axes, pairs[s]))
            return out

        def after(value, earlier):
            return lax.optimization_barrier((value, earlier))[0]

        forth = [[(i, shift_dest(i, s)) for i in range(n_dev)] for s in range(N_SHIFT)]
        back = [[(b, a) for a, b in pairs] for pairs in forth]
        split_pairs = [(i, split_partner(i)) for i in range(n_dev)]
        twin_pairs = [(i, twin_partner(i)) for i in range(n_dev)]

        order = []
        source = []
        for s in range(N_SHIFT):
            dx, dc, d = (s >> 2) & 1, (s >> 1) & 1, s & 1
            order.append(4 * (x ^ dx) + 2 * (c ^ dc) + (jnp.where((c ^ dc) == 0, y, z) ^ d))
            sx, sc = x ^ dx, c ^ dc
            sz = jnp.where(c == 0, z, z ^ d)
            sy = jnp.where(c == 0, y ^ d, y)
            source.append((sx * 2 + sc) * etp_size + sz * 2 + sy)
        order = jnp.stack(order).astype(I32)
        source = jnp.stack(source).astype(I32)

        ids_t = expert_ids.T
        slot_shape = jax.ShapeDtypeStruct((slots, d_model), BF16)
        slot_buf = pltpu.VMEM((n_experts, buf_rows, d_model), BF16)
        dma8 = pltpu.SemaphoreType.DMA((N_SHIFT,))
        spread_flops = 2 * tok_rows * n_experts * WIN * d_model

        def flip(value, bits):
            return lax.ppermute(value, dev_axes, [(i, i ^ bits) for i in range(n_dev)])

        steps = (2, 4, 8, 1)
        table = pl.pallas_call(
            count_kernel, in_specs=[vmem()], out_specs=vmem(), out_shape=jax.ShapeDtypeStruct((8, 128), I32), compiler_params=params(),
        )(ids_t)[:1]
        table = jnp.concatenate([table, flip(table, 2)])
        table = jnp.concatenate([table, flip(table, 4), flip(table, 8), flip(table, 12)])
        table = jnp.concatenate([table, flip(table, 1)])
        ids_peer, h_peer = flip(ids_t, 2), flip(hidden, 2)

        local_order = jnp.concatenate([order[:N_LOCAL], (4 * x)[None]])
        x_slots = pl.pallas_call(
            x_slots_kernel,
            in_specs=[smem(), vmem(), vmem()],
            out_specs=[vmem()] + [hbm()] * N_LOCAL,
            out_shape=[jax.ShapeDtypeStruct((n_experts, 128), I32)] + [slot_shape] * N_LOCAL,
            scratch_shapes=[pltpu.VMEM((N_LOCAL, buf_rows, d_model), BF16), pltpu.SMEM((n_experts, 128), I32), pltpu.SemaphoreType.DMA((N_LOCAL,)), pltpu.SemaphoreType.DMA],
            compiler_params=params(), cost_estimate=cost(spread_flops // 2, rows * d_model),
        )
        base, *x_own = x_slots(local_order, ids_t, hidden)
        _, *x_peer = x_slots(local_order, ids_peer, h_peer)
        x_recv = exchange(x_own, forth) + exchange(x_peer, forth)

        device = np.arange(n_dev)
        place = np.zeros(n_dev, np.int32)
        for step, bits in enumerate(steps):
            place += ((device & bits) != 0) << step
        by_block = [t * ep_size + o for o in range(ep_size) for t in range(etp_size)]
        me = etp * ep_size + ep
        count_table = jnp.take(table[:, :n_experts], jnp.take(jnp.asarray(place), jnp.asarray(by_block, I32) ^ me), axis=0)
        running = jnp.cumsum(count_table, axis=0) - count_table
        total_count = jnp.sum(count_table, axis=0)
        block_idx = ep * etp_size + etp
        limit = jnp.clip(capacity - running, 0, None)
        kept_table = jnp.minimum(count_table, limit)
        my_kept = kept_table[block_idx]
        my_expert = order[0]
        kept = kept_table[source, my_expert]
        part = (kept + ALIGN - 1) // ALIGN * ALIGN
        offset = jnp.concatenate([jnp.zeros((1,), I32), jnp.cumsum(part)]).astype(I32)
        n_tiles = (offset[N_SHIFT:] + ROW_TILE - 1) // ROW_TILE

        wr_t = split3(w_router.T)
        wr3 = jnp.concatenate(wr_t + (jnp.zeros_like(wr_t[0]),), axis=0)
        wr6 = jnp.concatenate([wr_t[0], wr_t[1], wr_t[0], wr_t[2], wr_t[1], wr_t[0], jnp.zeros((128 - 6 * n_experts, d_model), BF16)], axis=0)
        c_slots = pl.pallas_call(
            c_slots_kernel,
            in_specs=[smem()] * 2 + [vmem()] * 4,
            out_specs=[vmem()] * 2 + [hbm()] * N_SHIFT,
            out_shape=[jax.ShapeDtypeStruct((tok_rows, 128), F32), jax.ShapeDtypeStruct((n_experts, 128), F32)] + [slot_shape] * N_SHIFT,
            scratch_shapes=[slot_buf, pltpu.VMEM((n_experts, tok_rows), F32), dma8],
            compiler_params=params(), cost_estimate=cost(spread_flops, 2 * rows * d_model),
        )
        info, prob_sum, *c_send = c_slots(order, base, ids_t, hidden, d_out, wr3)

        def take(w, j):
            return lax.dynamic_index_in_dim(w, j, 0, keepdims=False)

        weights = (w_gate, w_up, w_down)
        q_own = [take(w, mine) for w in weights]
        q_twin = permute(q_own[:1], twin_pairs) + permute(q_own[1:], twin_pairs)
        q_split = permute([take(w, 1 - mine) for w in weights], split_pairs)
        q_far = permute(q_split, twin_pairs)

        c_recv = exchange(c_send, forth)

        def row_spec(w):
            return pl.BlockSpec((ROW_TILE, w), lambda i, n, *_: (jnp.clip(n[0] - 1, 0, i), 0))

        def full_spec(shape):
            return pl.BlockSpec(shape, lambda i, *_: (0, 0), pipeline_mode=pl.Buffered(1))

        grid = (rows // ROW_TILE,)
        up_shape, down_shape = (d_model, width), (width, d_model)
        row_f32 = jax.ShapeDtypeStruct((rows, d_model), F32)
        act_shape = jax.ShapeDtypeStruct((rows, width), F32)
        row_buf = pltpu.VMEM((rows + slots, d_model), BF16)
        mm = 2 * rows * d_model * width

        grad_shapes = [jax.ShapeDtypeStruct(up_shape, F32)] * 2 + [jax.ShapeDtypeStruct(down_shape, F32)]
        full = [full_spec(up_shape), full_spec(up_shape), full_spec(down_shape)]

        def rows_call(kernel, matmuls, ins, outs, shapes, scratch, aliases, *args, scalars=2):
            return pl.pallas_call(
                kernel,
                grid_spec=pltpu.PrefetchScalarGridSpec(num_scalar_prefetch=scalars, grid=grid, in_specs=ins, out_specs=outs, scratch_shapes=scratch),
                out_shape=shapes, input_output_aliases=aliases,
                compiler_params=params("arbitrary"), cost_estimate=cost(matmuls * mm, 20 * rows * d_model),
            )(n_tiles, offset, *args)

        slots_outs, slots_shapes, slots_scratch = [hbm()] * N_SHIFT, [slot_shape] * N_SHIFT, [row_buf, dma8]

        packed = jax.ShapeDtypeStruct((rows + ROW_TILE, d_model), BF16)
        pack_scratch = [pltpu.VMEM((rows + ROW_TILE, d_model), BF16), pltpu.SemaphoreType.DMA((N_SHIFT, 6)), pltpu.SemaphoreType.DMA((N_SHIFT + 1, 6))]

        def forward_first(quarter, parts):
            out = rows_call(
                forward_first_kernel, 3, [hbm()] * N_SHIFT + full, [row_spec(width)] * 2 + [row_spec(d_model), hbm()],
                [act_shape] * 2 + [row_f32, packed], pack_scratch, {}, kept, *parts, *quarter, scalars=3)
            return out[:2], out[2], out[3]

        def forward(quarter, y_acc, last=False):
            out = rows_call(
                functools.partial(forward_kernel, last=last), 3,
                [row_spec(d_model)] + full + [row_spec(d_model)], [row_spec(width)] * 2 + (slots_outs if last else [row_spec(d_model)]),
                [act_shape] * 2 + (slots_shapes if last else [row_f32]), slots_scratch if last else [], {} if last else {6: 2},
                x_rows, *quarter, y_acc)
            return out[:2], (out[2:] if last else out[2])

        def half(piece, pieces):
            w = width // pieces
            shapes = [(d_model, w), (d_model, w), (w, d_model)]
            act_spec = pl.BlockSpec((ROW_TILE, w), lambda i, n, *_: (jnp.clip(n[0] - 1, 0, i), piece))
            at = [(0, piece), (0, piece), (piece, 0)]
            w_specs = [pl.BlockSpec(shape, lambda i, *_, at=at: at, pipeline_mode=pl.Buffered(1)) for shape, at in zip(shapes, at)]
            return act_spec, w_specs, [full_spec(shape) for shape in shapes], [jax.ShapeDtypeStruct(shape, F32) for shape in shapes]

        def backward_first(quarter, acts, parts):
            act_spec, w_specs, g_specs, g_shapes = half(0, 2)
            out = rows_call(
                backward_first_kernel, 3, [hbm()] * N_SHIFT + [row_spec(d_model)] + [act_spec] * 2 + w_specs,
                g_specs + [row_spec(d_model), hbm()], g_shapes + [row_f32, packed], pack_scratch, {}, kept, *parts, x_rows, *acts, *quarter, scalars=3)
            return out[:3], out[3], out[4]

        def backward(quarter, acts, dx_acc, piece, pieces):
            act_spec, w_specs, g_specs, g_shapes = half(piece, pieces)
            out = rows_call(
                backward_kernel, 6 // pieces, [row_spec(d_model)] * 2 + [act_spec] * 2 + w_specs + [row_spec(d_model)],
                g_specs + [row_spec(d_model)], g_shapes + [row_f32], [], {9: 3}, x_rows, c_rows, *acts, *quarter, dx_acc)
            return out[:3], out[3]

        def both(quarter, y_acc, dx_acc):
            out = rows_call(
                both_kernel, 9, [row_spec(d_model)] * 2 + full + [row_spec(d_model)] * 2, full + [row_spec(d_model)] * 2,
                grad_shapes + [row_f32] * 2, [], {8: 3, 7: 4}, x_rows, c_rows, *quarter, y_acc, dx_acc)
            return out[:3], out[3], out[4]

        def backward_rows(quarter, acts, dx_acc):
            return rows_call(
                backward_rows_kernel, 3, [row_spec(d_model)] + [row_spec(width)] * 2 + full + [row_spec(d_model)], slots_outs,
                slots_shapes, slots_scratch, {}, c_rows, *acts, *quarter, dx_acc)

        def weight_grads(quarter, acts):
            return rows_call(
                weight_grads_kernel, 4, [row_spec(d_model)] * 2 + [row_spec(width)] * 2 + full[2:], full,
                grad_shapes, [], {}, x_rows, c_rows, *acts, quarter[2])

        act_own, acc_y, x_rows = forward_first(q_own, x_recv)
        act_twin, acc_y = forward(q_twin, acc_y)
        g_twin_0, acc_dx, c_rows = backward_first(q_twin, act_twin, [after(c_recv[0], acc_y)] + c_recv[1:])
        g_twin_0 = permute(g_twin_0, twin_pairs)
        g_twin_1, acc_dx = backward(q_twin, act_twin, acc_dx, 1, 2)
        g_twin_1 = permute(g_twin_1, twin_pairs)
        g_far, acc_dx, acc_y = both(q_far, acc_y, acc_dx)
        g_far = permute(g_far, twin_pairs)
        act_split, y_send = forward(q_split, acc_y, True)
        y_recv = exchange(y_send, back)
        g_split, acc_dx = backward(q_split, [after(act_split[0], acc_dx), act_split[1]], acc_dx, 0, 1)
        got_split = permute([g_split[0] + g_far[0]], split_pairs)
        dx_send = backward_rows(q_own, act_own, acc_dx)
        dx_recv = exchange(dx_send, back)

        g_split = got_split + permute([after(a, dx_send[0]) + b for a, b in zip(g_split[1:], g_far[1:])], split_pairs)
        g_own = weight_grads(q_own, [after(act_own[0], dx_send[0]), act_own[1]])
        route_frac = total_count.astype(F32) / (2 * n_tokens)
        aux_weight = (AUX_COEF * n_experts / n_tokens) * route_frac
        weight_row = jnp.concatenate([jnp.tile(aux_weight, 6), jnp.zeros((128 - 6 * n_experts,), F32)])[None, :]

        def tok_block(w):
            return pl.BlockSpec((TOK_TILE, w), lambda t: (t, 0))

        def whole(shape):
            return pl.BlockSpec(shape, lambda t: (0, 0))

        combine_scratch = [slot_buf, pltpu.VMEM((n_experts * WIN, d_model), BF16), dma8]
        y_combine = pl.pallas_call(
            y_combine_kernel, grid=(tok_rows // TOK_TILE,),
            in_specs=[smem()] * 3 + [hbm()] * N_SHIFT + [tok_block(128), tok_block(d_model), tok_block(d_model), whole((1, 128))],
            out_specs=[tok_block(d_model), tok_block(128), whole((128, d_model))],
            out_shape=[jax.ShapeDtypeStruct((tok_rows, d_model), BF16), jax.ShapeDtypeStruct((tok_rows, 128), BF16), jax.ShapeDtypeStruct((128, d_model), F32)],
            scratch_shapes=combine_scratch,
            compiler_params=params("arbitrary"), cost_estimate=cost(2 * spread_flops, 4 * rows * d_model),
        )
        output, dz, dwr = y_combine(order, base, my_kept, *y_recv, after(info, g_own[0]), hidden, d_out, weight_row)
        dwr_t = dwr[0:n_experts] + dwr[2 * n_experts:3 * n_experts] + dwr[5 * n_experts:6 * n_experts]
        shared = jnp.concatenate([dwr_t, jnp.pad(prob_sum, ((0, 0), (0, d_model - 128)))], axis=0)

        shared = shared + flip(shared, 1)
        across_x = flip(shared, 2)

        def finish_other(other, aliased):
            r, w = other.shape
            return pl.pallas_call(
                finish_other_kernel,
                grid_spec=pltpu.PrefetchScalarGridSpec(
                    num_scalar_prefetch=1, grid=(2,), in_specs=[pl.BlockSpec((r // 2, w), lambda i, j: (i, 0)), hbm()],
                    out_specs=pl.BlockSpec((1, r // 2, w), lambda i, j: (j[0] ^ 1, i, 0))),
                out_shape=jax.ShapeDtypeStruct((2, r, w), F32), input_output_aliases={2: 0},
                compiler_params=params("arbitrary"), cost_estimate=cost(10**9, 12 * r * w),
            )(mine[None].astype(I32), other, aliased)

        def finish_own(own, got_0, got_1):
            r, w = own.shape
            block = (r // 2, w) if got_0.shape[0] != r else (r, w // 2)
            place = (lambda i: (i, 0)) if got_0.shape[0] != r else (lambda i: (0, i))
            spec = pl.BlockSpec(block, lambda i, j: (0, 0), pipeline_mode=pl.Buffered(1))
            return pl.pallas_call(
                finish_own_kernel,
                grid_spec=pltpu.PrefetchScalarGridSpec(
                    num_scalar_prefetch=1, grid=(2,), in_specs=[pl.BlockSpec(block, lambda i, j: place(i)), spec, spec],
                    out_specs=pl.BlockSpec((1,) + block, lambda i, j: (j[0],) + place(i))),
                out_shape=jax.ShapeDtypeStruct((2, r, w), F32),
                compiler_params=params("arbitrary"), cost_estimate=cost(10**9, 12 * r * w),
            )(mine[None].astype(I32), own, got_0, got_1)

        halves = [finish_own(after(own, shared), got_0, got_1) for own, got_0, got_1 in zip(g_own, g_twin_0, g_twin_1)]
        d_hidden = pl.pallas_call(
            dx_combine_kernel, grid=(tok_rows // TOK_TILE,),
            in_specs=[smem()] * 3 + [hbm()] * N_SHIFT + [tok_block(128), tok_block(128), tok_block(d_model), whole((128, d_model))],
            out_specs=tok_block(d_model),
            out_shape=jax.ShapeDtypeStruct((tok_rows, d_model), BF16),
            scratch_shapes=combine_scratch,
            compiler_params=params("arbitrary"), cost_estimate=cost(spread_flops, 4 * rows * d_model),
        )(order, base, my_kept, *dx_recv, after(info, halves), dz, d_out, wr6)

        shared = shared + after(across_x, d_hidden)
        across = [flip(shared, bits) for bits in (4, 8, 12)]
        done = d_hidden
        outputs = []
        for other, half in zip(g_split, halves):
            done = finish_other(after(other, done), half)
            outputs.append(done)
        d_gate, d_up, d_down = outputs
        across = [after(v, d_down) for v in across]
        shared = (shared + across[0]) + (across[1] + across[2])
        d_router = shared[:n_experts].T
        prob_total = shared[n_experts:, 0]
        aux_loss = AUX_COEF * n_experts * jnp.sum(route_frac * (prob_total / n_tokens))
        return output, d_hidden, d_router, aux_loss, d_gate, d_up, d_down

    return jax.shard_map(layer, mesh=mesh, in_specs=(tok_spec, P(), tok_spec, tok_spec, gate_spec, gate_spec, down_spec), out_specs=(tok_spec, tok_spec, P(), P(), gate_spec, gate_spec, down_spec), check_vma=False)
```

```python
import functools
import jax
import jax.numpy as jnp
import numpy as np
from jax import lax
from jax.experimental import pallas as pl
from jax.experimental.pallas import tpu as pltpu
from jax.sharding import PartitionSpec as P


AUX_COEF = 0.01
OUT_SCALE = 2.0
BF16 = jnp.bfloat16
F32 = jnp.float32
I32 = jnp.int32
VMEM_LIMIT = 62 * 1024 * 1024


N_SHIFT = 8
N_LOCAL = 4
TOK_TILE = 256
ROW_TILE = 512
ALIGN = 16
WIN = TOK_TILE + ALIGN


def coords(i):
    return (i >> 3) & 1, (i >> 2) & 1, (i >> 1) & 1, i & 1


def index_of(z, y, x, c):
    return (z << 3) | (y << 2) | (x << 1) | c


def shift_dest(i, s):
    z, y, x, c = coords(i)
    x, c, d = x ^ ((s >> 2) & 1), c ^ ((s >> 1) & 1), s & 1
    return index_of(z, y ^ d, x, c) if c == 0 else index_of(z ^ d, y, x, c)


def split_partner(i):
    z, y, x, c = coords(i)
    return index_of(z, y ^ 1, x, c) if c == 0 else index_of(z ^ 1, y, x, c)


def twin_partner(i):
    z, y, x, c = coords(i)
    return index_of(z ^ 1, y, x, c) if c == 0 else index_of(z, y ^ 1, x, c)


def dot_nn(a, b):
    return lax.dot_general(a, b, (((1,), (0,)), ((), ())), preferred_element_type=F32)


def dot_nt(a, b):
    return lax.dot_general(a, b, (((1,), (1,)), ((), ())), preferred_element_type=F32)


def dot_tn(a, b):
    return lax.dot_general(a, b, (((0,), (0,)), ((), ())), preferred_element_type=F32)


def val(ref):
    return ref[...]


def ones_where(condition):
    return jnp.where(condition, 1.0, 0.0).astype(BF16)


def iota(shape, dim):
    return lax.broadcasted_iota(I32, shape, dim)


def tile_columns(ids_t, starts, n_experts, upper, first=0):
    tokens = ids_t.shape[1]
    e_iota = iota((n_experts, tokens), 0) + first
    hot0 = ids_t[0:1, :] == e_iota
    hot1 = ids_t[1:2, :] == e_iota
    either = ones_where(hot0 | hot1)
    before = dot_nn(either, upper).astype(I32)
    offset = jnp.zeros((n_experts, tokens), I32)
    for e in range(n_experts):
        offset = jnp.where(e_iota == first + e, e * WIN + (starts[e] & (ALIGN - 1)), offset)
    column = before + offset + 1
    return [jnp.sum(jnp.where(hot, column, 0), axis=0, keepdims=True) - 1 for hot in (hot0, hot1)]


def strict_upper(n):
    return ones_where(iota((n, n), 0) < iota((n, n), 1))


def add_windows(buf, value, starts, n_experts):
    for e in range(n_experts):
        rows = pl.ds(pl.multiple_of(starts[e] - (starts[e] & (ALIGN - 1)), ALIGN), WIN)
        buf[e, rows, :] = buf[e, rows, :] + value[e * WIN:(e + 1) * WIN, :]


def slots_out(buf, order_ref, outs, sem, first=0):
    slots = outs[0].shape[0]
    copies = [pltpu.make_async_copy(buf.at[order_ref[s] - first, pl.ds(0, slots), :], out, sem.at[s]) for s, out in enumerate(outs)]
    for copy in copies:
        copy.start()
    for copy in copies:
        copy.wait()


def count_kernel(ids_ref, out_ref):
    tokens = ids_ref.shape[1]
    e_iota = iota((128, tokens), 0)
    hot = (ids_ref[0:1, :] == e_iota) | (ids_ref[1:2, :] == e_iota)
    out_ref[...] = dot_nt(jnp.ones((8, tokens), BF16), ones_where(hot)).astype(I32)


def x_slots_kernel(order_ref, ids_ref, h_ref, base_ref, *rest):
    outs, (buf, base_s, sem, base_sem) = rest[:N_LOCAL], rest[N_LOCAL:]
    n_experts, tokens = base_ref.shape[0], ids_ref.shape[1]
    lowest = order_ref[N_LOCAL]
    e_iota = iota((n_experts, tokens), 0)
    hot = (ids_ref[0:1, :] == e_iota) | (ids_ref[1:2, :] == e_iota)
    earlier = ones_where(iota((tokens, 128), 0) < TOK_TILE * iota((tokens, 128), 1))
    base_ref[...] = dot_nn(ones_where(hot), earlier).astype(I32)
    copy = pltpu.make_async_copy(base_ref, base_s, base_sem)
    copy.start()
    buf[...] = jnp.zeros_like(buf)
    copy.wait()
    upper = strict_upper(TOK_TILE)

    @pl.loop(0, tokens // TOK_TILE)
    def _(t):
        here = pl.ds(pl.multiple_of(t * TOK_TILE, TOK_TILE), TOK_TILE)
        starts = [base_s[lowest + e, t] for e in range(N_LOCAL)]
        col0, col1 = tile_columns(ids_ref[:, here], starts, N_LOCAL, upper, lowest)
        row = iota((N_LOCAL * WIN, TOK_TILE), 0)
        pick = ones_where((row == col0) | (row == col1))
        add_windows(buf, dot_nn(pick, h_ref[here, :]).astype(BF16), starts, N_LOCAL)

    slots_out(buf, order_ref, outs, sem, lowest)


def c_slots_kernel(order_ref, base_s, ids_ref, h_ref, dy_ref, wr3_ref, info_ref, psum_ref, *rest):
    outs, (buf, prob_buf, sem) = rest[:N_SHIFT], rest[N_SHIFT:]
    n_experts, tokens = psum_ref.shape[0], ids_ref.shape[1]
    parts = dot_nt(val(wr3_ref), val(h_ref))
    logits = parts[2 * n_experts:3 * n_experts] + parts[n_experts:2 * n_experts] + parts[0:n_experts]
    top = jnp.max(logits, axis=0, keepdims=True)
    expo = jnp.exp(logits - top)
    prob = expo / jnp.sum(expo, axis=0, keepdims=True)
    prob_buf[...] = prob
    psum_ref[...] = jnp.broadcast_to(jnp.sum(prob, axis=1, keepdims=True), psum_ref.shape)
    buf[...] = jnp.zeros_like(buf)
    upper = strict_upper(TOK_TILE)

    @pl.loop(0, tokens // TOK_TILE)
    def _(t):
        here = pl.ds(pl.multiple_of(t * TOK_TILE, TOK_TILE), TOK_TILE)
        starts = [base_s[e, t] for e in range(n_experts)]
        ids_t = ids_ref[:, here]
        p_t = prob_buf[:, here]
        e_iota = iota((n_experts, TOK_TILE), 0)
        p0 = jnp.sum(jnp.where(ids_t[0:1, :] == e_iota, p_t, 0.0), axis=0, keepdims=True)
        p1 = jnp.sum(jnp.where(ids_t[1:2, :] == e_iota, p_t, 0.0), axis=0, keepdims=True)
        total = p0 + p1
        g0, g1 = p0 / total, p1 / total
        col0, col1 = tile_columns(ids_t, starts, n_experts, upper)
        row = iota((n_experts * WIN, TOK_TILE), 0)
        is0, is1 = row == col0, row == col1
        pick = ones_where(is0 | is1)
        gate = jnp.sum(jnp.where(is0, g0, jnp.where(is1, g1, 0.0)), axis=1, keepdims=True)
        mixed = OUT_SCALE * dot_nn(pick, dy_ref[here, :])
        add_windows(buf, (gate * mixed).astype(BF16), starts, n_experts)
        group = iota((8, TOK_TILE), 0)
        extra = jnp.zeros((8, TOK_TILE), F32)
        for k, v in enumerate((g0, g1, col0.astype(F32), col1.astype(F32), ids_t[0:1, :].astype(F32), ids_t[1:2, :].astype(F32))):
            extra = jnp.where(group == k, v, extra)
        table = jnp.concatenate([p_t] * 6 + [extra, jnp.zeros((128 - 6 * n_experts - 8, TOK_TILE), F32)], axis=0)
        info_ref[here, :] = table.T

    slots_out(buf, order_ref, outs, sem)


def pack_rows(kept_s, offset_s, ins, out_ref, buf, sem, out_sem):
    sizes = [512, 256, 128, 64, 32, 16]

    def for_parts(s, act):
        offset = offset_s[s]
        count = offset_s[s + 1] - offset
        done = jnp.int32(0)
        for j, size in enumerate(sizes):
            has = (count & size) != 0
            start = pl.multiple_of(done, ALIGN)
            dest = pl.multiple_of(offset + done, ALIGN)

            @pl.when(has)
            def _(j=j, size=size, start=start, dest=dest):
                rows = pl.ds(dest, size)
                act(lambda: pltpu.make_async_copy(ins[s].at[pl.ds(start, size), :], buf.at[rows, :], sem.at[s, j]),
                    lambda: pltpu.make_async_copy(buf.at[rows, :], out_ref.at[rows, :], out_sem.at[s, j]))

            done = done + jnp.where(has, size, 0)

    def tail_copy():
        tail = pl.ds(pl.multiple_of(offset_s[N_SHIFT], ALIGN), ROW_TILE)
        return tail, pltpu.make_async_copy(buf.at[tail, :], out_ref.at[tail, :], out_sem.at[N_SHIFT, 0])

    def begin():
        for s in range(N_SHIFT):
            for_parts(s, lambda load, store: load().start())
        tail, copy = tail_copy()
        buf[tail, :] = jnp.zeros((ROW_TILE, buf.shape[1]), buf.dtype)
        for s in range(N_SHIFT):
            for_parts(s, lambda load, store: load().wait())
            extra = kept_s[s] & (ALIGN - 1)

            @pl.when(extra != 0)
            def _(s=s, extra=extra):
                group = pl.ds(pl.multiple_of(offset_s[s] + kept_s[s] - extra, ALIGN), ALIGN)
                rows = buf[group, :]
                buf[group, :] = jnp.where(iota(rows.shape, 0) < extra, rows, jnp.zeros_like(rows))

            for_parts(s, lambda load, store: store().start())
        copy.start()

    def end():
        for s in range(N_SHIFT):
            for_parts(s, lambda load, store: store().wait())
        tail_copy()[1].wait()

    pl.when(pl.program_id(0) == 0)(begin)
    return lambda: pl.when(pl.program_id(0) == pl.num_programs(0) - 1)(end)


def rows_out(buf, offset_s, outs, sem):
    slots = outs[0].shape[0]
    copies = [pltpu.make_async_copy(buf.at[pl.ds(pl.multiple_of(offset_s[s], ALIGN), slots), :], outs[s], sem.at[s]) for s in range(N_SHIFT)]
    for copy in copies:
        copy.start()
    for copy in copies:
        copy.wait()


def clear(refs):
    @pl.when(pl.program_id(0) == 0)
    def _():
        for ref in refs:
            ref[...] = jnp.zeros_like(ref)


def row_tile(buf):
    return buf[pl.ds(pl.multiple_of(pl.program_id(0) * ROW_TILE, ROW_TILE), ROW_TILE), :]


def forward_first_kernel(n_ref, offset_s, kept_s, *refs, quarters):
    ins, refs = refs[:N_SHIFT], refs[N_SHIFT:]
    weights, refs = refs[:3 * quarters], refs[3 * quarters:]
    acts, refs = refs[:2 * quarters], refs[2 * quarters:]
    y_out, rows_ref, buf, sem, out_sem = refs
    end = pack_rows(kept_s, offset_s, ins, rows_ref, buf, sem, out_sem)

    @pl.when(pl.program_id(0) < n_ref[0])
    def _():
        x = row_tile(buf)
        total = None
        for q in range(quarters):
            w1_ref, w3_ref, w2_ref = weights[3 * q:3 * q + 3]
            a = dot_nn(x, val(w1_ref))
            b = dot_nn(x, val(w3_ref))
            acts[2 * q][...] = a
            acts[2 * q + 1][...] = b
            y = dot_nn((a * jax.nn.sigmoid(a) * b).astype(BF16), val(w2_ref))
            total = y if total is None else total + y
        y_out[...] = total

    end()


def forward_last_kernel(n_ref, offset_s, x_ref, w1_ref, w3_ref, w2_ref, y_in, a_ref, b_ref, *rest):
    outs, (buf, sem) = rest[:N_SHIFT], rest[N_SHIFT:]
    i = pl.program_id(0)

    @pl.when(i < n_ref[0])
    def _():
        a = dot_nn(val(x_ref), val(w1_ref))
        b = dot_nn(val(x_ref), val(w3_ref))
        a_ref[...] = a
        b_ref[...] = b
        y = val(y_in) + dot_nn((a * jax.nn.sigmoid(a) * b).astype(BF16), val(w2_ref))
        buf[pl.ds(pl.multiple_of(i * ROW_TILE, ROW_TILE), ROW_TILE), :] = y.astype(BF16)

    @pl.when(i == pl.num_programs(0) - 1)
    def _():
        rows_out(buf, offset_s, outs, sem)


def act_grads(du, a, b):
    sig = jax.nn.sigmoid(a)
    silu = a * sig
    da = (du * b * sig * (1.0 + a * (1.0 - sig))).astype(BF16)
    return da, (du * silu).astype(BF16), (silu * b).astype(BF16)


def add_weight_grads(x, c, da, db, u, g1_ref, g3_ref, g2_ref):
    g1_ref[...] += dot_tn(x, da)
    g3_ref[...] += dot_tn(x, db)
    g2_ref[...] += dot_tn(u, c)


def backward_first_kernel(n_ref, offset_s, kept_s, *refs):
    ins, refs = refs[:N_SHIFT], refs[N_SHIFT:]
    x_ref, a_ref, b_ref, w1_ref, w3_ref, w2_ref, g1_ref, g3_ref, g2_ref, dx_out, rows_ref, buf, sem, out_sem = refs
    clear((g1_ref, g3_ref, g2_ref))
    end = pack_rows(kept_s, offset_s, ins, rows_ref, buf, sem, out_sem)

    @pl.when(pl.program_id(0) < n_ref[0])
    def _():
        c = row_tile(buf)
        da, db, u = act_grads(dot_nt(c, val(w2_ref)), val(a_ref), val(b_ref))
        dx_out[...] = dot_nt(da, val(w1_ref)) + dot_nt(db, val(w3_ref))
        add_weight_grads(val(x_ref), c, da, db, u, g1_ref, g3_ref, g2_ref)

    end()


def backward_kernel(n_ref, offset_s, x_ref, c_ref, a_ref, b_ref, w1_ref, w3_ref, w2_ref, dx_in, g1_ref, g3_ref, g2_ref, dx_out):
    clear((g1_ref, g3_ref, g2_ref))

    @pl.when(pl.program_id(0) < n_ref[0])
    def _():
        da, db, u = act_grads(dot_nt(val(c_ref), val(w2_ref)), val(a_ref), val(b_ref))
        dx_out[...] = val(dx_in) + (dot_nt(da, val(w1_ref)) + dot_nt(db, val(w3_ref)))
        add_weight_grads(val(x_ref), val(c_ref), da, db, u, g1_ref, g3_ref, g2_ref)


def both_kernel(n_ref, offset_s, x_ref, c_ref, w1_ref, w3_ref, w2_ref, y_in, dx_in, g1_ref, g3_ref, g2_ref, dx_out, y_out):
    clear((g1_ref, g3_ref, g2_ref))

    @pl.when(pl.program_id(0) < n_ref[0])
    def _():
        x, c = val(x_ref), val(c_ref)
        a = dot_nn(x, val(w1_ref))
        b = dot_nn(x, val(w3_ref))
        da, db, u = act_grads(dot_nt(c, val(w2_ref)), a, b)
        y_out[...] = val(y_in) + dot_nn(u, val(w2_ref))
        dx_out[...] = val(dx_in) + (dot_nt(da, val(w1_ref)) + dot_nt(db, val(w3_ref)))
        add_weight_grads(x, c, da, db, u, g1_ref, g3_ref, g2_ref)


def backward_rows_kernel(n_ref, offset_s, c_ref, a_ref, b_ref, w1_ref, w3_ref, w2_ref, dx_in, *rest):
    outs, (buf, sem) = rest[:N_SHIFT], rest[N_SHIFT:]
    i = pl.program_id(0)

    @pl.when(i < n_ref[0])
    def _():
        da, db, _ = act_grads(dot_nt(val(c_ref), val(w2_ref)), val(a_ref), val(b_ref))
        dx = val(dx_in) + (dot_nt(da, val(w1_ref)) + dot_nt(db, val(w3_ref)))
        buf[pl.ds(pl.multiple_of(i * ROW_TILE, ROW_TILE), ROW_TILE), :] = dx.astype(BF16)

    @pl.when(i == pl.num_programs(0) - 1)
    def _():
        rows_out(buf, offset_s, outs, sem)


def weight_grads_kernel(n_ref, offset_s, x_ref, c_ref, a_ref, b_ref, w2_ref, g1_ref, g3_ref, g2_ref):
    clear((g1_ref, g3_ref, g2_ref))

    @pl.when(pl.program_id(0) < n_ref[0])
    def _():
        da, db, u = act_grads(dot_nt(val(c_ref), val(w2_ref)), val(a_ref), val(b_ref))
        add_weight_grads(val(x_ref), val(c_ref), da, db, u, g1_ref, g3_ref, g2_ref)


def load_slots(order_ref, ins, buf, sem):
    slots = ins[0].shape[0]
    copies = [pltpu.make_async_copy(ins[s], buf.at[order_ref[s], pl.ds(0, slots), :], sem.at[s]) for s in range(N_SHIFT)]
    for copy in copies:
        copy.start()
    for copy in copies:
        copy.wait()


def gather_windows(buf, window, base_s, kept_s, t, n_experts):
    for e in range(n_experts):
        start = base_s[e, t] - (base_s[e, t] & (ALIGN - 1))
        rows = buf[e, pl.ds(pl.multiple_of(start, ALIGN), WIN), :]
        valid = iota(rows.shape, 0) < kept_s[e] - start
        window[e * WIN:(e + 1) * WIN, :] = jnp.where(valid, rows, jnp.zeros_like(rows))


def y_combine_kernel(order_ref, base_s, kept_s, *refs):
    ins, refs = refs[:N_SHIFT], refs[N_SHIFT:]
    info_ref, h_ref, dy_ref, w_ref, out_ref, dz_ref, dwr_ref, buf, window, sem = refs
    n_experts = buf.shape[0]
    t = pl.program_id(0)

    @pl.when(t == 0)
    def _():
        load_slots(order_ref, ins, buf, sem)
        dwr_ref[...] = jnp.zeros_like(dwr_ref)

    gather_windows(buf, window, base_s, kept_s, t, n_experts)
    info = val(info_ref)
    k0 = 6 * n_experts
    g0, g1, col0, col1, e0, e1 = [info[:, k0 + k:k0 + k + 1] for k in range(6)]
    col = iota((TOK_TILE, n_experts * WIN), 1)
    pick0 = ones_where(col == col0.astype(I32))
    pick1 = ones_where(col == col1.astype(I32))
    y0 = dot_nn(pick0, val(window))
    y1 = dot_nn(pick1, val(window))
    h = val(h_ref)
    mix = OUT_SCALE * val(dy_ref).astype(F32)
    out_ref[...] = (h.astype(F32) + OUT_SCALE * (g0 * y0 + g1 * y1)).astype(BF16)
    dg0 = jnp.sum(mix * y0, axis=1, keepdims=True)
    dg1 = jnp.sum(mix * y1, axis=1, keepdims=True)
    lane = iota(info.shape, 1)
    prob = jnp.where(lane < k0, info, 0.0)
    weight = val(w_ref)
    mean_w = jnp.sum(jnp.where(lane < n_experts, prob * weight, 0.0), axis=1, keepdims=True)
    expert = (lane & (n_experts - 1)).astype(F32)
    sign = jnp.where(expert == e0, 1.0, 0.0) - jnp.where(expert == e1, 1.0, 0.0)
    dz = prob * (weight - mean_w) + g0 * g1 * (dg0 - dg1) * jnp.where(lane < k0, sign, 0.0)
    d1 = dz.astype(BF16)
    rem1 = dz - d1.astype(F32)
    d2 = rem1.astype(BF16)
    d3 = (rem1 - d2.astype(F32)).astype(BF16)
    group = lane // n_experts
    first = (group == 0) | (group == 1) | (group == 3)
    second = (group == 2) | (group == 4)
    dzp = jnp.where(first, d1.astype(F32), jnp.where(second, d2.astype(F32), d3.astype(F32))).astype(BF16)
    dz_ref[...] = dzp
    dwr_ref[...] += dot_tn(dzp, h)


def dx_combine_kernel(order_ref, base_s, kept_s, *refs):
    ins, refs = refs[:N_SHIFT], refs[N_SHIFT:]
    info_ref, dz_ref, dy_ref, wr_ref, out_ref, buf, window, sem = refs
    n_experts = buf.shape[0]
    t = pl.program_id(0)

    @pl.when(t == 0)
    def _():
        load_slots(order_ref, ins, buf, sem)

    gather_windows(buf, window, base_s, kept_s, t, n_experts)
    info = val(info_ref)
    k0 = 6 * n_experts
    col0, col1 = info[:, k0 + 2:k0 + 3].astype(I32), info[:, k0 + 3:k0 + 4].astype(I32)
    col = iota((TOK_TILE, n_experts * WIN), 1)
    pick = ones_where((col == col0) | (col == col1))
    total = val(dy_ref).astype(F32) + dot_nn(pick, val(window)) + dot_nn(val(dz_ref), val(wr_ref))
    out_ref[...] = total.astype(BF16)


def finish_own_kernel(j_ref, own_ref, part_0_ref, part_1_ref, out_ref):
    for piece, part_ref in enumerate((part_0_ref, part_1_ref)):
        @pl.when(pl.program_id(0) == piece)
        def _(part_ref=part_ref):
            out_ref[0] = val(own_ref) + val(part_ref)


def finish_other_kernel(j_ref, other_ref, _, out_ref):
    out_ref[0] = val(other_ref)


def params(*semantics):
    return pltpu.CompilerParams(dimension_semantics=semantics or None, vmem_limit_bytes=VMEM_LIMIT)


def hbm():
    return pl.BlockSpec(memory_space=pl.ANY)


def smem():
    return pl.BlockSpec(memory_space=pltpu.SMEM)


def vmem():
    return pl.BlockSpec(memory_space=pltpu.VMEM)


def cost(flops, nbytes):
    return pl.CostEstimate(flops=int(flops), bytes_accessed=int(nbytes), transcendentals=0)


def split3(v):
    p1 = v.astype(BF16)
    r1 = v - p1.astype(F32)
    p2 = r1.astype(BF16)
    return p1, p2, (r1 - p2.astype(F32)).astype(BF16)


def solution(mesh):
    ep_size = mesh.shape["ep"]
    etp_size = mesh.shape["etp"]
    n_dev = ep_size * etp_size
    all_axes = ("ep", "etp")
    dev_axes = ("etp", "ep")
    tok_spec = P(all_axes, None)
    gate_spec = P("ep", None, "etp")
    down_spec = P("ep", "etp", None)

    def layer(hidden, w_router, expert_ids, d_out, w_gate, w_up, w_down):
        tok_rows, d_model = hidden.shape
        n_experts = w_router.shape[1]
        n_tokens = tok_rows * n_dev
        capacity = (5 * n_tokens + 2 * n_experts - 1) // (2 * n_experts)
        slots = 7 * tok_rows // (2 * n_experts)
        width = w_gate.shape[2]
        rows = N_SHIFT * slots
        buf_rows = slots + WIN + ALIGN
        etp, ep = lax.axis_index("etp"), lax.axis_index("ep")
        z, y, x, c = etp >> 1, etp & 1, ep >> 1, ep & 1
        mine = jnp.where(c == 0, y, z)

        def permute(values, pairs):
            return [lax.ppermute(v, dev_axes, pairs) for v in values]

        def exchange(parts, pairs):
            out = [parts[0]]
            for s in range(1, len(parts)):
                out.append(lax.ppermute(parts[s], dev_axes, pairs[s]))
            return out

        def after(value, earlier):
            return lax.optimization_barrier((value, earlier))[0]

        forth = [[(i, shift_dest(i, s)) for i in range(n_dev)] for s in range(N_SHIFT)]
        back = [[(b, a) for a, b in pairs] for pairs in forth]
        split_pairs = [(i, split_partner(i)) for i in range(n_dev)]
        twin_pairs = [(i, twin_partner(i)) for i in range(n_dev)]

        order = []
        source = []
        for s in range(N_SHIFT):
            dx, dc, d = (s >> 2) & 1, (s >> 1) & 1, s & 1
            order.append(4 * (x ^ dx) + 2 * (c ^ dc) + (jnp.where((c ^ dc) == 0, y, z) ^ d))
            sx, sc = x ^ dx, c ^ dc
            sz = jnp.where(c == 0, z, z ^ d)
            sy = jnp.where(c == 0, y ^ d, y)
            source.append((sx * 2 + sc) * etp_size + sz * 2 + sy)
        order = jnp.stack(order).astype(I32)
        source = jnp.stack(source).astype(I32)

        ids_t = expert_ids.T
        slot_shape = jax.ShapeDtypeStruct((slots, d_model), BF16)
        slot_buf = pltpu.VMEM((n_experts, buf_rows, d_model), BF16)
        dma8 = pltpu.SemaphoreType.DMA((N_SHIFT,))
        spread_flops = 2 * tok_rows * n_experts * WIN * d_model

        def flip(value, bits):
            return lax.ppermute(value, dev_axes, [(i, i ^ bits) for i in range(n_dev)])

        steps = (2, 4, 8, 1)
        table = pl.pallas_call(
            count_kernel, in_specs=[vmem()], out_specs=vmem(), out_shape=jax.ShapeDtypeStruct((8, 128), I32), compiler_params=params(),
        )(ids_t)[:1]
        table = jnp.concatenate([table, flip(table, 2)])
        table = jnp.concatenate([table, flip(table, 4), flip(table, 8), flip(table, 12)])
        table = jnp.concatenate([table, flip(table, 1)])
        ids_peer, h_peer = flip(ids_t, 2), flip(hidden, 2)

        local_order = jnp.concatenate([order[:N_LOCAL], (4 * x)[None]])
        x_slots = pl.pallas_call(
            x_slots_kernel,
            in_specs=[smem(), vmem(), vmem()],
            out_specs=[vmem()] + [hbm()] * N_LOCAL,
            out_shape=[jax.ShapeDtypeStruct((n_experts, 128), I32)] + [slot_shape] * N_LOCAL,
            scratch_shapes=[pltpu.VMEM((N_LOCAL, buf_rows, d_model), BF16), pltpu.SMEM((n_experts, 128), I32), pltpu.SemaphoreType.DMA((N_LOCAL,)), pltpu.SemaphoreType.DMA],
            compiler_params=params(), cost_estimate=cost(spread_flops // 2, rows * d_model),
        )
        base, *x_own = x_slots(local_order, ids_t, hidden)
        _, *x_peer = x_slots(local_order, ids_peer, h_peer)
        x_recv = exchange(x_own, forth) + exchange(x_peer, forth)

        device = np.arange(n_dev)
        place = np.zeros(n_dev, np.int32)
        for step, bits in enumerate(steps):
            place += ((device & bits) != 0) << step
        by_block = [t * ep_size + o for o in range(ep_size) for t in range(etp_size)]
        me = etp * ep_size + ep
        count_table = jnp.take(table[:, :n_experts], jnp.take(jnp.asarray(place), jnp.asarray(by_block, I32) ^ me), axis=0)
        running = jnp.cumsum(count_table, axis=0) - count_table
        total_count = jnp.sum(count_table, axis=0)
        block_idx = ep * etp_size + etp
        limit = jnp.clip(capacity - running, 0, None)
        kept_table = jnp.minimum(count_table, limit)
        my_kept = kept_table[block_idx]
        my_expert = order[0]
        kept = kept_table[source, my_expert]
        part = (kept + ALIGN - 1) // ALIGN * ALIGN
        offset = jnp.concatenate([jnp.zeros((1,), I32), jnp.cumsum(part)]).astype(I32)
        n_tiles = (offset[N_SHIFT:] + ROW_TILE - 1) // ROW_TILE

        wr_t = split3(w_router.T)
        wr3 = jnp.concatenate(wr_t + (jnp.zeros_like(wr_t[0]),), axis=0)
        wr6 = jnp.concatenate([wr_t[0], wr_t[1], wr_t[0], wr_t[2], wr_t[1], wr_t[0], jnp.zeros((128 - 6 * n_experts, d_model), BF16)], axis=0)
        c_slots = pl.pallas_call(
            c_slots_kernel,
            in_specs=[smem()] * 2 + [vmem()] * 4,
            out_specs=[vmem()] * 2 + [hbm()] * N_SHIFT,
            out_shape=[jax.ShapeDtypeStruct((tok_rows, 128), F32), jax.ShapeDtypeStruct((n_experts, 128), F32)] + [slot_shape] * N_SHIFT,
            scratch_shapes=[slot_buf, pltpu.VMEM((n_experts, tok_rows), F32), dma8],
            compiler_params=params(), cost_estimate=cost(spread_flops, 2 * rows * d_model),
        )
        info, prob_sum, *c_send = c_slots(order, base, ids_t, hidden, d_out, wr3)

        def take(w, j):
            return lax.dynamic_index_in_dim(w, j, 0, keepdims=False)

        weights = (w_gate, w_up, w_down)
        q_own = [take(w, mine) for w in weights]
        q_twin = permute(q_own, twin_pairs)
        q_other = [take(w, 1 - mine) for w in weights]
        q_split = permute(q_other[:1], split_pairs) + permute(q_other[1:], split_pairs)
        q_far = permute(q_split[:1], twin_pairs) + permute(q_split[1:], twin_pairs)

        c_recv = exchange(c_send, forth)

        def row_spec(w):
            return pl.BlockSpec((ROW_TILE, w), lambda i, n, *_: (jnp.clip(n[0] - 1, 0, i), 0))

        def full_spec(shape):
            return pl.BlockSpec(shape, lambda i, *_: (0, 0), pipeline_mode=pl.Buffered(1))

        grid = (rows // ROW_TILE,)
        up_shape, down_shape = (d_model, width), (width, d_model)
        row_f32 = jax.ShapeDtypeStruct((rows, d_model), F32)
        act_shape = jax.ShapeDtypeStruct((rows, width), F32)
        row_buf = pltpu.VMEM((rows + slots, d_model), BF16)
        mm = 2 * rows * d_model * width

        grad_shapes = [jax.ShapeDtypeStruct(up_shape, F32)] * 2 + [jax.ShapeDtypeStruct(down_shape, F32)]
        full = [full_spec(up_shape), full_spec(up_shape), full_spec(down_shape)]

        def rows_call(kernel, matmuls, ins, outs, shapes, scratch, aliases, *args, scalars=2):
            return pl.pallas_call(
                kernel,
                grid_spec=pltpu.PrefetchScalarGridSpec(num_scalar_prefetch=scalars, grid=grid, in_specs=ins, out_specs=outs, scratch_shapes=scratch),
                out_shape=shapes, input_output_aliases=aliases,
                compiler_params=params("arbitrary"), cost_estimate=cost(matmuls * mm, 20 * rows * d_model),
            )(n_tiles, offset, *args)

        slots_outs, slots_shapes, slots_scratch = [hbm()] * N_SHIFT, [slot_shape] * N_SHIFT, [row_buf, dma8]

        packed = jax.ShapeDtypeStruct((rows + ROW_TILE, d_model), BF16)
        pack_scratch = [pltpu.VMEM((rows + ROW_TILE, d_model), BF16), pltpu.SemaphoreType.DMA((N_SHIFT, 6)), pltpu.SemaphoreType.DMA((N_SHIFT + 1, 6))]

        def forward_first(quarters, parts):
            k = len(quarters)
            flat = [w for quarter in quarters for w in quarter]
            out = rows_call(
                functools.partial(forward_first_kernel, quarters=k), 3 * k, [hbm()] * N_SHIFT + full * k, [row_spec(width)] * (2 * k) + [row_spec(d_model), hbm()],
                [act_shape] * (2 * k) + [row_f32, packed], pack_scratch, {}, kept, *parts, *flat, scalars=3)
            return [out[2 * q:2 * q + 2] for q in range(k)], out[-2], out[-1]

        def forward_last(quarter, y_acc):
            out = rows_call(
                forward_last_kernel, 3, [row_spec(d_model)] + full + [row_spec(d_model)], [row_spec(width)] * 2 + slots_outs,
                [act_shape] * 2 + slots_shapes, slots_scratch, {}, x_rows, *quarter, y_acc)
            return out[:2], out[2:]

        def half(piece, pieces):
            w = width // pieces
            shapes = [(d_model, w), (d_model, w), (w, d_model)]
            act_spec = pl.BlockSpec((ROW_TILE, w), lambda i, n, *_: (jnp.clip(n[0] - 1, 0, i), piece))
            at = [(0, piece), (0, piece), (piece, 0)]
            w_specs = [pl.BlockSpec(shape, lambda i, *_, at=at: at, pipeline_mode=pl.Buffered(1)) for shape, at in zip(shapes, at)]
            return act_spec, w_specs, [full_spec(shape) for shape in shapes], [jax.ShapeDtypeStruct(shape, F32) for shape in shapes]

        def backward_first(quarter, acts, parts):
            act_spec, w_specs, g_specs, g_shapes = half(0, 2)
            out = rows_call(
                backward_first_kernel, 3, [hbm()] * N_SHIFT + [row_spec(d_model)] + [act_spec] * 2 + w_specs,
                g_specs + [row_spec(d_model), hbm()], g_shapes + [row_f32, packed], pack_scratch, {}, kept, *parts, x_rows, *acts, *quarter, scalars=3)
            return out[:3], out[3], out[4]

        def backward(quarter, acts, dx_acc, piece, pieces):
            act_spec, w_specs, g_specs, g_shapes = half(piece, pieces)
            out = rows_call(
                backward_kernel, 6 // pieces, [row_spec(d_model)] * 2 + [act_spec] * 2 + w_specs + [row_spec(d_model)],
                g_specs + [row_spec(d_model)], g_shapes + [row_f32], [], {9: 3}, x_rows, c_rows, *acts, *quarter, dx_acc)
            return out[:3], out[3]

        def both(quarter, y_acc, dx_acc):
            out = rows_call(
                both_kernel, 9, [row_spec(d_model)] * 2 + full + [row_spec(d_model)] * 2, full + [row_spec(d_model)] * 2,
                grad_shapes + [row_f32] * 2, [], {8: 3, 7: 4}, x_rows, c_rows, *quarter, y_acc, dx_acc)
            return out[:3], out[3], out[4]

        def backward_rows(quarter, acts, dx_acc):
            return rows_call(
                backward_rows_kernel, 3, [row_spec(d_model)] + [row_spec(width)] * 2 + full + [row_spec(d_model)], slots_outs,
                slots_shapes, slots_scratch, {}, c_rows, *acts, *quarter, dx_acc)

        def weight_grads(quarter, acts):
            return rows_call(
                weight_grads_kernel, 4, [row_spec(d_model)] * 2 + [row_spec(width)] * 2 + full[2:], full,
                grad_shapes, [], {}, x_rows, c_rows, *acts, quarter[2])

        (act_own, act_twin), acc_y, x_rows = forward_first([q_own, q_twin], x_recv)
        g_twin_0, acc_dx, c_rows = backward_first(q_twin, act_twin, [after(c_recv[0], acc_y)] + c_recv[1:])
        g_twin_0 = permute(g_twin_0, twin_pairs)
        g_twin_1, acc_dx = backward(q_twin, act_twin, acc_dx, 1, 2)
        g_twin_1 = permute(g_twin_1, twin_pairs)
        g_far, acc_dx, acc_y = both(q_far, acc_y, acc_dx)
        g_far = permute(g_far[:1], twin_pairs) + permute(g_far[1:], twin_pairs)
        act_split, y_send = forward_last(q_split, acc_y)
        y_recv = exchange(y_send, back)
        g_split, acc_dx = backward(q_split, [after(act_split[0], acc_dx), act_split[1]], acc_dx, 0, 1)
        got_split = permute([g_split[0] + g_far[0]], split_pairs)
        dx_send = backward_rows(q_own, act_own, acc_dx)
        dx_recv = exchange(dx_send, back)

        g_split = got_split + permute([after(a, dx_send[0]) + b for a, b in zip(g_split[1:], g_far[1:])], split_pairs)
        g_own = weight_grads(q_own, [after(act_own[0], dx_send[0]), act_own[1]])
        route_frac = total_count.astype(F32) / (2 * n_tokens)
        aux_weight = (AUX_COEF * n_experts / n_tokens) * route_frac
        weight_row = jnp.concatenate([jnp.tile(aux_weight, 6), jnp.zeros((128 - 6 * n_experts,), F32)])[None, :]

        def tok_block(w):
            return pl.BlockSpec((TOK_TILE, w), lambda t: (t, 0))

        def whole(shape):
            return pl.BlockSpec(shape, lambda t: (0, 0))

        combine_scratch = [slot_buf, pltpu.VMEM((n_experts * WIN, d_model), BF16), dma8]
        y_combine = pl.pallas_call(
            y_combine_kernel, grid=(tok_rows // TOK_TILE,),
            in_specs=[smem()] * 3 + [hbm()] * N_SHIFT + [tok_block(128), tok_block(d_model), tok_block(d_model), whole((1, 128))],
            out_specs=[tok_block(d_model), tok_block(128), whole((128, d_model))],
            out_shape=[jax.ShapeDtypeStruct((tok_rows, d_model), BF16), jax.ShapeDtypeStruct((tok_rows, 128), BF16), jax.ShapeDtypeStruct((128, d_model), F32)],
            scratch_shapes=combine_scratch,
            compiler_params=params("arbitrary"), cost_estimate=cost(2 * spread_flops, 4 * rows * d_model),
        )
        output, dz, dwr = y_combine(order, base, my_kept, *y_recv, after(info, g_own[0]), hidden, d_out, weight_row)
        dwr_t = dwr[0:n_experts] + dwr[2 * n_experts:3 * n_experts] + dwr[5 * n_experts:6 * n_experts]
        shared = jnp.concatenate([dwr_t, jnp.pad(prob_sum, ((0, 0), (0, d_model - 128)))], axis=0)

        shared = shared + flip(shared, 1)
        across_x = flip(shared, 2)

        def finish_other(other, aliased):
            r, w = other.shape
            return pl.pallas_call(
                finish_other_kernel,
                grid_spec=pltpu.PrefetchScalarGridSpec(
                    num_scalar_prefetch=1, grid=(2,), in_specs=[pl.BlockSpec((r // 2, w), lambda i, j: (i, 0)), hbm()],
                    out_specs=pl.BlockSpec((1, r // 2, w), lambda i, j: (j[0] ^ 1, i, 0))),
                out_shape=jax.ShapeDtypeStruct((2, r, w), F32), input_output_aliases={2: 0},
                compiler_params=params("arbitrary"), cost_estimate=cost(10**9, 12 * r * w),
            )(mine[None].astype(I32), other, aliased)

        def finish_own(own, got_0, got_1):
            r, w = own.shape
            block = (r // 2, w) if got_0.shape[0] != r else (r, w // 2)
            place = (lambda i: (i, 0)) if got_0.shape[0] != r else (lambda i: (0, i))
            spec = pl.BlockSpec(block, lambda i, j: (0, 0), pipeline_mode=pl.Buffered(1))
            return pl.pallas_call(
                finish_own_kernel,
                grid_spec=pltpu.PrefetchScalarGridSpec(
                    num_scalar_prefetch=1, grid=(2,), in_specs=[pl.BlockSpec(block, lambda i, j: place(i)), spec, spec],
                    out_specs=pl.BlockSpec((1,) + block, lambda i, j: (j[0],) + place(i))),
                out_shape=jax.ShapeDtypeStruct((2, r, w), F32),
                compiler_params=params("arbitrary"), cost_estimate=cost(10**9, 12 * r * w),
            )(mine[None].astype(I32), own, got_0, got_1)

        halves = [finish_own(after(own, shared), got_0, got_1) for own, got_0, got_1 in zip(g_own, g_twin_0, g_twin_1)]
        d_gate = finish_other(g_split[0], halves[0])

        d_hidden = pl.pallas_call(
            dx_combine_kernel, grid=(tok_rows // TOK_TILE,),
            in_specs=[smem()] * 3 + [hbm()] * N_SHIFT + [tok_block(128), tok_block(128), tok_block(d_model), whole((128, d_model))],
            out_specs=tok_block(d_model),
            out_shape=jax.ShapeDtypeStruct((tok_rows, d_model), BF16),
            scratch_shapes=combine_scratch,
            compiler_params=params("arbitrary"), cost_estimate=cost(spread_flops, 4 * rows * d_model),
        )(order, base, my_kept, *dx_recv, after(info, d_gate), dz, d_out, wr6)

        shared = shared + after(across_x, d_hidden)
        across = [flip(shared, bits) for bits in (4, 8, 12)]
        d_up, d_down = [finish_other(after(other, d_hidden), part) for other, part in zip(g_split[1:], halves[1:])]
        across = [after(v, d_down) for v in across]
        shared = (shared + across[0]) + (across[1] + across[2])
        d_router = shared[:n_experts].T
        prob_total = shared[n_experts:, 0]
        aux_loss = AUX_COEF * n_experts * jnp.sum(route_frac * (prob_total / n_tokens))
        return output, d_hidden, d_router, aux_loss, d_gate, d_up, d_down

    return jax.shard_map(layer, mesh=mesh, in_specs=(tok_spec, P(), tok_spec, tok_spec, gate_spec, gate_spec, down_spec), out_specs=(tok_spec, tok_spec, P(), P(), gate_spec, gate_spec, down_spec), check_vma=False)
```
